64 devices in a mesh: rep: 4 (over x, y), dp: 16 (over z, core).
Axes of the slice: x: 2, y: 2, z: 8, core: 2. Of those that a mesh axis runs over, the one named last changes fastest.
The devices are a block of a 4x4x8 slice.
Arguments:
- g_w_gate: bfloat16 [64, 2, 640, 2048], P(('rep', 'dp')), parts along dimension 0
- g_w_up: bfloat16 [64, 2, 640, 2048], P(('rep', 'dp')), parts along dimension 0
- g_w_down: bfloat16 [64, 2, 2048, 640], P(('rep', 'dp')), parts along dimension 0
- w_gate: bfloat16 [2, 640, 2048], replicated
- w_up: bfloat16 [2, 640, 2048], replicated
- w_down: bfloat16 [2, 2048, 640], replicated
- m_w_gate: float32 [2, 640, 2048], P(None, 'dp')
- m_w_up: float32 [2, 640, 2048], P(None, 'dp')
- m_w_down: float32 [2, 2048, 640], P(None, 'dp')
- v_w_gate: float32 [2, 640, 2048], P(None, 'dp')
- v_w_up: float32 [2, 640, 2048], P(None, 'dp')
- v_w_down: float32 [2, 2048, 640], P(None, 'dp')
Outputs:
- output 1: bfloat16 [8, 640, 2048], P('rep'), parts along dimension 0
- output 2: bfloat16 [8, 640, 2048], P('rep'), parts along dimension 0
- output 3: bfloat16 [8, 2048, 640], P('rep'), parts along dimension 0
- output 4: float32 [8, 640, 2048], P('rep', 'dp'), parts along dimension 0
- output 5: float32 [8, 640, 2048], P('rep', 'dp'), parts along dimension 0
- output 6: float32 [8, 2048, 640], P('rep', 'dp'), parts along dimension 0
- output 7: float32 [8, 640, 2048], P('rep', 'dp'), parts along dimension 0
- output 8: float32 [8, 640, 2048], P('rep', 'dp'), parts along dimension 0
- output 9: float32 [8, 2048, 640], P('rep', 'dp'), parts along dimension 0
There are 4 independent parts. The reference program is written for one: setup_inputs(seed, part) draws one part's arguments, and reference() takes and returns one part's arrays. A program takes and returns all parts, laid end to end along the dimension named above; an argument that names none is the same for every part.
All inputs are finite; a program needn't handle non-finite values.
Results may differ from the reference program's by a relative error of at most 0.022.
Values are sent between devices in bfloat16 or wider.
A program may use at most 768 MiB of HBM per device.

```python
import jax
import jax.numpy as jnp
from jax import lax

DEVICES = 16
D = 640
FF = 2048
LAYERS = 2
NAMES = ("w_gate", "w_up", "w_down")
SHAPES = {"w_gate": (LAYERS, D, FF), "w_up": (LAYERS, D, FF), "w_down": (LAYERS, FF, D)}


def setup_inputs(seed: int = 0, part: int = 0) -> dict:
    kz, *keys = jax.random.split(jax.random.key(seed), 1 + 5 * len(NAMES))
    loud = 2.0 ** jax.random.uniform(kz, (), jnp.float32, -1.0, 1.0)
    drawn = {}
    for name, key, both in zip(NAMES, keys[:3], keys[3:6], strict=True):
        own = jax.random.normal(jax.random.fold_in(key, part), (DEVICES, *SHAPES[name]), jnp.float32)
        shared = jax.random.normal(jax.random.fold_in(both, part), SHAPES[name], jnp.float32)
        drawn["g_" + name] = (loud * (0.7 * shared / DEVICES + 0.7 * own * DEVICES**-0.5)).astype(jnp.bfloat16)
    for name, key in zip(NAMES, keys[6:9], strict=True):
        drawn[name] = (jax.random.normal(key, SHAPES[name], jnp.float32) * SHAPES[name][1] ** -0.5).astype(jnp.bfloat16)
    for name, key in zip(NAMES, keys[9:12], strict=True):
        drawn["m_" + name] = loud * 0.5 * jax.random.normal(key, SHAPES[name], jnp.float32)
    for name, key in zip(NAMES, keys[12:15], strict=True):
        drawn["v_" + name] = loud * loud * jax.random.uniform(key, SHAPES[name], jnp.float32, 0.5, 1.5)
    return drawn


def adamw(w, m, v, g):
    m = 0.9 * m + 0.1 * g
    v = 0.95 * v + 0.05 * g * g
    step = m * lax.rsqrt(v + 1e-8) + 0.1 * w
    return (w - 0.02 * step).astype(jnp.bfloat16), m, v


def reference(g_w_gate, g_w_up, g_w_down, w_gate, w_up, w_down, m_w_gate, m_w_up, m_w_down, v_w_gate, v_w_up, v_w_down):
    def total(terms):
        return lax.scan(lambda so_far, term: (so_far + term.astype(jnp.float32), None), jnp.zeros(terms.shape[1:], jnp.float32), terms)[0]

    gradients = [total(terms).astype(jnp.bfloat16).astype(jnp.float32) for terms in (g_w_gate, g_w_up, g_w_down)]
    new = [
        adamw(w.astype(jnp.float32), m, v, g)
        for w, m, v, g in zip((w_gate, w_up, w_down), (m_w_gate, m_w_up, m_w_down), (v_w_gate, v_w_up, v_w_down), gradients, strict=True)
    ]
    return tuple(one[which] for which in range(3) for one in new)
```

```python
import functools

import jax
import jax.numpy as jnp
from jax import lax
from jax.experimental import pallas as pl
from jax.experimental.pallas import tpu as pltpu
from jax.sharding import PartitionSpec as P

MESH = pl.DeviceIdType.MESH
CORES = 2
SUBLANES = 8


def adamw(w, m, v, g):
    m = 0.9 * m + 0.1 * g
    v = 0.95 * v + 0.05 * g * g
    step = m * lax.rsqrt(v + 1e-8) + 0.1 * w
    return (w - 0.02 * step).astype(jnp.bfloat16), m, v


def kernel(n, chips, layers, *refs):
    refs = iter(refs)
    take = lambda count: [next(refs) for _ in range(count)]
    g, w, m_in, v_in = take(n), take(n), take(n), take(n)
    new_w, new_m, new_v = take(n), take(n), take(n)
    own, pair, ring, old_w = take(n), take(n), take(n), take(n)
    (load_sem, state_sem, pair_recv, ring_recv, gather_recv, share_recv, pair_send, ring_send, gather_send, share_send) = take(10)

    me = lax.axis_index("dp")
    chip, core = me // CORES, me % CORES
    other = 1 - core
    partner = {"dp": chip * CORES + other}
    right = {"dp": (chip + 1) % chips * CORES + core}
    left = {"dp": (chip + chips - 1) % chips * CORES + core}
    ahead = [right if layer % 2 == 0 else left for layer in range(layers)]

    def block(step, layer):
        return (chip + chips - 1 - step if layer % 2 == 0 else chip + 1 + step) % chips

    def source(step, layer):
        return (chip + chips - step if layer % 2 == 0 else chip + step) % chips

    pieces = [(a, layer) for a in range(n) for layer in range(layers)]

    def load(a, step, layer):
        return pltpu.make_async_copy(g[a].at[layer, block(step, layer), core], own[a].at[step, layer], load_sem.at[a, step, layer])

    def swap(a, step, layer):
        return pltpu.make_async_remote_copy(
            g[a].at[layer, block(step, layer), other], pair[a].at[step, layer], pair_send.at[a], pair_recv.at[a, step, layer], partner, MESH
        )

    def hop(a, step, layer):
        return pltpu.make_async_remote_copy(
            own[a].at[step, layer], ring[a].at[step, layer], ring_send.at[a], ring_recv.at[a, step, layer], ahead[layer], MESH
        )

    def spread(a, step, layer):
        here = new_w[a].at[layer, source(step, layer), core]
        return pltpu.make_async_remote_copy(here, here, gather_send.at[a], gather_recv.at[a, step, layer], ahead[layer], MESH)

    def share(a, step, layer):
        here = new_w[a].at[layer, source(step, layer), core]
        return pltpu.make_async_remote_copy(here, here, share_send.at[a], share_recv.at[a], partner, MESH)

    def states(a):
        return [
            pltpu.make_async_copy(m_in[a], new_m[a], state_sem.at[0, a]),
            pltpu.make_async_copy(v_in[a], new_v[a], state_sem.at[1, a]),
        ] + [pltpu.make_async_copy(w[a].at[layer, chip, core], old_w[a].at[layer], state_sem.at[2 + layer, a]) for layer in range(layers)]

    @pl.loop(0, chips)
    def _(step):
        for a, layer in pieces:
            load(a, step, layer).start()

    barrier = pltpu.get_barrier_semaphore()
    for device in (partner, right, left):
        pl.semaphore_signal(barrier, inc=1, device_id=device, device_id_type=MESH)
    pl.semaphore_wait(barrier, 3)

    @pl.loop(0, chips)
    def _(step):
        for a, layer in pieces:
            swap(a, step, layer).start()

    for a in range(n):
        for copy in states(a):
            copy.start()

    def total(a, step, layer, i, arrived):
        t = own[a][step, layer, i].astype(jnp.float32) + pair[a][step, layer, i].astype(jnp.float32)
        if arrived is not None:
            t = t + ring[a][arrived, layer, i].astype(jnp.float32)
        return t

    def pair_sum(step, arrived):
        for a, layer in pieces:
            load(a, step, layer).wait()
            swap(a, step, layer).wait_recv()
            if arrived is not None:
                hop(a, arrived, layer).wait_recv()

            @pl.loop(0, own[a].shape[2])
            def _(i):
                own[a][step, layer, i] = total(a, step, layer, i, arrived).astype(jnp.bfloat16)

            hop(a, step, layer).start()

    pair_sum(0, None)

    @pl.loop(1, chips - 1)
    def _(step):
        pair_sum(step, step - 1)

    last = chips - 1
    for a in range(n):
        for copy in states(a):
            copy.wait()
    for a, layer in pieces:
        load(a, last, layer).wait()
        swap(a, last, layer).wait_recv()
        hop(a, last - 1, layer).wait_recv()

        @pl.loop(0, own[a].shape[2])
        def _(i):
            grad = total(a, last, layer, i, last - 1).astype(jnp.bfloat16).astype(jnp.float32)
            new = adamw(old_w[a][layer, i].astype(jnp.float32), new_m[a][layer, i], new_v[a][layer, i], grad)
            new_w[a][layer, chip, core, i], new_m[a][layer, i], new_v[a][layer, i] = new

        spread(a, 0, layer).start()
        share(a, 0, layer).start()

    @pl.loop(1, chips - 1)
    def _(step):
        for a, layer in pieces:
            spread(a, step - 1, layer).wait_recv()
            spread(a, step, layer).start()
            share(a, step, layer).start()

    for a, layer in pieces:
        spread(a, last - 1, layer).wait_recv()
        share(a, last, layer).start()

    for a in range(n):
        pltpu.make_async_remote_copy(pair[a], pair[a], pair_send.at[a], share_recv.at[a], partner, MESH).wait_send()
        pltpu.make_async_remote_copy(ring[a], ring[a], ring_send.at[a], share_recv.at[a], partner, MESH).wait_send()
        pltpu.make_async_remote_copy(ring[a], ring[a], gather_send.at[a], share_recv.at[a], partner, MESH).wait_send()
        pltpu.make_async_remote_copy(pair[a], pair[a], share_send.at[a], share_recv.at[a], partner, MESH).wait()


def solution(mesh):
    chips = mesh.shape["dp"] // CORES

    def step(*arrays):
        terms, weights, m, v = (arrays[i : i + 3] for i in (0, 3, 6, 9))
        n, layers = len(terms), weights[0].shape[0]
        tiles = [(one.shape[1] // SUBLANES, SUBLANES, one.shape[2]) for one in m]
        whole = [(layers, chips, CORES, *tile) for tile in tiles]
        state = [(layers, *tile) for tile in tiles]
        operands = [one.reshape(shape) for one, shape in zip(terms, whole, strict=True)]
        operands += [one.reshape(shape) for one, shape in zip(weights, whole, strict=True)]
        operands += [one.reshape(shape) for part in (m, v) for one, shape in zip(part, state, strict=True)]
        sems = lambda *shape: pltpu.SemaphoreType.DMA(shape)
        vmem = lambda lead, dtype: [pltpu.VMEM((*lead, *tile), dtype) for tile in tiles]
        out = pl.pallas_call(
            functools.partial(kernel, n, chips, layers),
            out_shape=[pltpu.VMEM(shape, jnp.bfloat16) for shape in whole] + [pltpu.VMEM(shape, jnp.float32) for shape in state] * 2,
            in_specs=[pl.BlockSpec(memory_space=pl.ANY)] * len(operands),
            out_specs=[pl.BlockSpec(memory_space=pltpu.VMEM)] * (3 * n),
            scratch_shapes=[
                *vmem((chips, layers), jnp.bfloat16),
                *vmem((chips, layers), jnp.bfloat16),
                *vmem((chips - 1, layers), jnp.bfloat16),
                *vmem((layers,), jnp.bfloat16),
                sems(n, chips, layers),
                sems(2 + layers, n),
                sems(n, chips, layers),
                sems(n, chips - 1, layers),
                sems(n, chips - 1, layers),
                sems(n),
                sems(n),
                sems(n),
                sems(n),
                sems(n),
            ],
            compiler_params=pltpu.CompilerParams(collective_id=0, has_side_effects=True, vmem_limit_bytes=40 << 20),
            name="step",
        )(*operands)
        return tuple(one.reshape(like.shape) for one, like in zip(out, (*weights, *m, *v), strict=True))

    all_of, cut = P(None, None, None), P(None, "dp", None)
    return jax.shard_map(
        step,
        mesh=mesh,
        in_specs=(P(("rep", "dp"), None, None, None),) * 3 + (all_of,) * 3 + (cut,) * 6,
        out_specs=(P("rep", None, None),) * 3 + (P("rep", "dp", None),) * 6,
        check_vma=False,
    )
```

```python
import functools

import jax
import jax.numpy as jnp
from jax import lax
from jax.experimental import pallas as pl
from jax.experimental.pallas import tpu as pltpu
from jax.sharding import PartitionSpec as P

MESH = pl.DeviceIdType.MESH
CORES = 2
SUBLANES = 8


def adamw(w, m, v, g):
    m = 0.9 * m + 0.1 * g
    v = 0.95 * v + 0.05 * g * g
    step = m * lax.rsqrt(v + 1e-8) + 0.1 * w
    return (w - 0.02 * step).astype(jnp.bfloat16), m, v


def kernel(n, chips, layers, *refs):
    refs = iter(refs)
    take = lambda count: [next(refs) for _ in range(count)]
    g, w, m_in, v_in = take(n), take(n), take(n), take(n)
    new_w, new_m, new_v = take(n), take(n), take(n)
    own, pair, ring, stage, old_w = take(n), take(n), take(n), take(n), take(n)
    (load_sem, stage_sem, state_sem, pair_recv, ring_recv, gather_recv, share_recv, stage_send, pair_send, ring_send, gather_send, share_send) = take(12)

    me = lax.axis_index("dp")
    chip, core = me // CORES, me % CORES
    other = 1 - core
    partner = {"dp": chip * CORES + other}
    right = {"dp": (chip + 1) % chips * CORES + core}
    left = {"dp": (chip + chips - 1) % chips * CORES + core}
    ahead = [right if layer % 2 == 0 else left for layer in range(layers)]

    def block(step, layer):
        return (chip + chips - 1 - step if layer % 2 == 0 else chip + 1 + step) % chips

    def source(step, layer):
        return (chip + chips - step if layer % 2 == 0 else chip + step) % chips

    pieces = [(a, layer) for a in range(n) for layer in range(layers)]

    def load(a, step, layer):
        return pltpu.make_async_copy(g[a].at[layer, block(step, layer), core], own[a].at[step, layer], load_sem.at[a, step, layer])

    def prepare(a, layer):
        return pltpu.make_async_copy(g[a].at[layer, block(0, layer), other], stage[a].at[layer], stage_sem.at[a, layer])

    def first_swap(a, layer):
        return pltpu.make_async_remote_copy(
            stage[a].at[layer], pair[a].at[0, layer], stage_send.at[a], pair_recv.at[a, 0, layer], partner, MESH
        )

    def swap(a, step, layer):
        return pltpu.make_async_remote_copy(
            g[a].at[layer, block(step, layer), other], pair[a].at[step, layer], pair_send.at[a], pair_recv.at[a, step, layer], partner, MESH
        )

    def hop(a, step, layer):
        return pltpu.make_async_remote_copy(
            own[a].at[step, layer], ring[a].at[step, layer], ring_send.at[a], ring_recv.at[a, step, layer], ahead[layer], MESH
        )

    def spread(a, step, layer):
        here = new_w[a].at[layer, source(step, layer), core]
        return pltpu.make_async_remote_copy(here, here, gather_send.at[a], gather_recv.at[a, step, layer], ahead[layer], MESH)

    def share(a, step, layer):
        here = new_w[a].at[layer, source(step, layer), core]
        return pltpu.make_async_remote_copy(here, here, share_send.at[a], share_recv.at[a], partner, MESH)

    def states(a):
        return [
            pltpu.make_async_copy(m_in[a], new_m[a], state_sem.at[0, a]),
            pltpu.make_async_copy(v_in[a], new_v[a], state_sem.at[1, a]),
        ] + [pltpu.make_async_copy(w[a].at[layer, chip, core], old_w[a].at[layer], state_sem.at[2 + layer, a]) for layer in range(layers)]

    barrier = pltpu.get_barrier_semaphore()
    for device in (partner, right, left):
        pl.semaphore_signal(barrier, inc=1, device_id=device, device_id_type=MESH)
    for a, layer in pieces:
        prepare(a, layer).start()
        load(a, 0, layer).start()

    @pl.loop(1, chips)
    def _(step):
        for a, layer in pieces:
            load(a, step, layer).start()

    pl.semaphore_wait(barrier, 3)
    for a, layer in pieces:
        prepare(a, layer).wait()
        first_swap(a, layer).start()

    @pl.loop(1, chips)
    def _(step):
        for a, layer in pieces:
            swap(a, step, layer).start()

    def total(a, step, layer, i, arrived):
        t = own[a][step, layer, i].astype(jnp.float32) + pair[a][step, layer, i].astype(jnp.float32)
        if arrived is not None:
            t = t + ring[a][arrived, layer, i].astype(jnp.float32)
        return t

    def pair_sum(step, arrived):
        for a, layer in pieces:
            load(a, step, layer).wait()
            swap(a, step, layer).wait_recv()
            if arrived is not None:
                hop(a, arrived, layer).wait_recv()

            @pl.loop(0, own[a].shape[2])
            def _(i):
                own[a][step, layer, i] = total(a, step, layer, i, arrived).astype(jnp.bfloat16)

            hop(a, step, layer).start()

    pair_sum(0, None)
    for a in range(n):
        for copy in states(a):
            copy.start()

    @pl.loop(1, chips - 1)
    def _(step):
        pair_sum(step, step - 1)

    last = chips - 1
    for a in range(n):
        for copy in states(a):
            copy.wait()
    for a, layer in pieces:
        load(a, last, layer).wait()
        swap(a, last, layer).wait_recv()
        hop(a, last - 1, layer).wait_recv()

        @pl.loop(0, own[a].shape[2])
        def _(i):
            grad = total(a, last, layer, i, last - 1).astype(jnp.bfloat16).astype(jnp.float32)
            new = adamw(old_w[a][layer, i].astype(jnp.float32), new_m[a][layer, i], new_v[a][layer, i], grad)
            new_w[a][layer, chip, core, i], new_m[a][layer, i], new_v[a][layer, i] = new

        spread(a, 0, layer).start()
        share(a, 0, layer).start()

    @pl.loop(1, chips - 1)
    def _(step):
        for a, layer in pieces:
            spread(a, step - 1, layer).wait_recv()
            spread(a, step, layer).start()
            share(a, step, layer).start()

    for a, layer in pieces:
        spread(a, last - 1, layer).wait_recv()
        share(a, last, layer).start()

    for a in range(n):
        pltpu.make_async_remote_copy(stage[a], stage[a], stage_send.at[a], share_recv.at[a], partner, MESH).wait_send()
        pltpu.make_async_remote_copy(ring[a], ring[a], pair_send.at[a], share_recv.at[a], partner, MESH).wait_send()
        pltpu.make_async_remote_copy(ring[a], ring[a], ring_send.at[a], share_recv.at[a], partner, MESH).wait_send()
        pltpu.make_async_remote_copy(ring[a], ring[a], gather_send.at[a], share_recv.at[a], partner, MESH).wait_send()
        pltpu.make_async_remote_copy(pair[a], pair[a], share_send.at[a], share_recv.at[a], partner, MESH).wait()


def write(count, *refs):
    sources, targets, sem = refs[:count], refs[count:-1], refs[-1]
    copies = [
        pltpu.make_async_copy(source.at[i], target.at[i], sem.at[k, i])
        for k, (source, target) in enumerate(zip(sources, targets, strict=True))
        for i in range(source.shape[0])
    ]
    for copy in copies:
        copy.start()
    for copy in copies:
        copy.wait()


def solution(mesh):
    chips = mesh.shape["dp"] // CORES

    def step(*arrays):
        terms, weights, m, v = (arrays[i : i + 3] for i in (0, 3, 6, 9))
        n, layers = len(terms), weights[0].shape[0]
        tiles = [(one.shape[1] // SUBLANES, SUBLANES, one.shape[2]) for one in m]
        whole = [(layers, chips, CORES, *tile) for tile in tiles]
        state = [(layers, *tile) for tile in tiles]
        operands = [one.reshape(shape) for one, shape in zip(terms, whole, strict=True)]
        operands += [one.reshape(shape) for one, shape in zip(weights, whole, strict=True)]
        operands += [one.reshape(shape) for part in (m, v) for one, shape in zip(part, state, strict=True)]
        sems = lambda *shape: pltpu.SemaphoreType.DMA(shape)
        vmem = lambda lead, dtype: [pltpu.VMEM((*lead, *tile), dtype) for tile in tiles]
        out = pl.pallas_call(
            functools.partial(kernel, n, chips, layers),
            out_shape=[pltpu.VMEM(shape, jnp.bfloat16) for shape in whole] + [pltpu.VMEM(shape, jnp.float32) for shape in state] * 2,
            in_specs=[pl.BlockSpec(memory_space=pl.ANY)] * len(operands),
            out_specs=[pl.BlockSpec(memory_space=pltpu.VMEM)] * (3 * n),
            scratch_shapes=[
                *vmem((chips, layers), jnp.bfloat16),
                *vmem((chips, layers), jnp.bfloat16),
                *vmem((chips - 1, layers), jnp.bfloat16),
                *vmem((layers,), jnp.bfloat16),
                *vmem((layers,), jnp.bfloat16),
                sems(n, chips, layers),
                sems(n, layers),
                sems(2 + layers, n),
                sems(n, chips, layers),
                sems(n, chips - 1, layers),
                sems(n, chips - 1, layers),
                *[sems(n)] * 6,
            ],
            compiler_params=pltpu.CompilerParams(collective_id=0, has_side_effects=True, vmem_limit_bytes=40 << 20),
            name="step",
        )(*operands)
        out = pl.pallas_call(
            functools.partial(write, len(out)),
            out_shape=[jax.ShapeDtypeStruct(one.shape, one.dtype) for one in out],
            in_specs=[pl.BlockSpec(memory_space=pltpu.VMEM)] * len(out),
            out_specs=[pl.BlockSpec(memory_space=pl.ANY)] * len(out),
            scratch_shapes=[sems(len(out), layers)],
            compiler_params=pltpu.CompilerParams(vmem_limit_bytes=1 << 20),
            name="write",
        )(*[pltpu.with_memory_space_constraint(one, pltpu.VMEM) for one in out])
        return tuple(one.reshape(like.shape) for one, like in zip(out, (*weights, *m, *v), strict=True))

    all_of, cut = P(None, None, None), P(None, "dp", None)
    return jax.shard_map(
        step,
        mesh=mesh,
        in_specs=(P(("rep", "dp"), None, None, None),) * 3 + (all_of,) * 3 + (cut,) * 6,
        out_specs=(P("rep", None, None),) * 3 + (P("rep", "dp", None),) * 6,
        check_vma=False,
    )
```

```python
import functools

import jax
import jax.numpy as jnp
from jax import lax
from jax.experimental import pallas as pl
from jax.experimental.pallas import tpu as pltpu
from jax.sharding import PartitionSpec as P

MESH = pl.DeviceIdType.MESH
CORES = 2
SUBLANES = 8


def adamw(w, m, v, g):
    m = 0.9 * m + 0.1 * g
    v = 0.95 * v + 0.05 * g * g
    step = m * lax.rsqrt(v + 1e-8) + 0.1 * w
    return (w - 0.02 * step).astype(jnp.bfloat16), m, v


def kernel(n, chips, layers, *refs):
    refs = iter(refs)
    take = lambda count: [next(refs) for _ in range(count)]
    g, w, m_in, v_in = take(n), take(n), take(n), take(n)
    new_w, new_m, new_v = take(n), take(n), take(n)
    own, pair, ring, stage, old_w = take(n), take(n), take(n), take(n), take(n)
    load_sem, stage_sem, state_sem, first_recv, pair_recv, ring_recv, share_recv, swap_send, ring_send = take(9)

    me = lax.axis_index("dp")
    chip, core = me // CORES, me % CORES
    other = 1 - core
    last = chips - 1
    partner = {"dp": chip * CORES + other}
    to = [1 - 2 * ((layer + core) % 2) for layer in range(layers)]
    ahead = [{"dp": (chip + chips + d) % chips * CORES + core} for d in to]
    pieces = [(a, layer) for a in range(n) for layer in range(layers)]

    def block(step, way):
        return (chip + 2 * chips - way * (step + 1)) % chips

    def source(step, layer):
        return (chip + chips - to[layer] * step) % chips

    def load(a, step, layer):
        return pltpu.make_async_copy(g[a].at[layer, block(step, to[layer]), core], own[a].at[step, layer], load_sem.at[a, step % 2])

    def prepare(a, layer):
        return pltpu.make_async_copy(g[a].at[layer, block(0, -to[layer]), other], stage[a].at[layer], stage_sem.at[a])

    def first_swap(a, layer):
        return pltpu.make_async_remote_copy(
            stage[a].at[layer], pair[a].at[0, layer], swap_send.at[a], first_recv.at[a, layer], partner, MESH
        )

    def swap(a, step, layer):
        return pltpu.make_async_remote_copy(
            g[a].at[layer, block(step, -to[layer]), other], pair[a].at[step, layer], swap_send.at[a], pair_recv.at[a, step - 1], partner, MESH
        )

    def hop(a, step, layer):
        return pltpu.make_async_remote_copy(
            own[a].at[step, layer], ring[a].at[step, layer], ring_send.at[a], ring_recv.at[a, step, layer], ahead[layer], MESH
        )

    def spread(a, step, layer):
        here = new_w[a].at[layer, source(step, layer), core]
        return pltpu.make_async_remote_copy(
            here, here, ring_send.at[a], ring_recv.at[a, (step + last) % chips, layer], ahead[layer], MESH
        )

    def share(a, step, layer):
        here = new_w[a].at[layer, source(step, layer), core]
        return pltpu.make_async_remote_copy(here, here, swap_send.at[a], share_recv.at[a], partner, MESH)

    def wait_both(here, sem):
        pltpu.make_async_copy(here, here, sem).wait()

    def take_own(a, step):
        wait_both(own[a].at[step], load_sem.at[a, step % 2])

    def take_pair(a, step):
        wait_both(pair[a].at[step], pair_recv.at[a, step - 1])

    def fetch(step):
        for a, layer in pieces:
            swap(a, step, layer).start()
        for a, layer in pieces:
            load(a, step, layer).start()

    barrier = pltpu.get_barrier_semaphore()
    for device in (*(dict(dp=(chip + d) % chips * CORES + core) for d in (1, last)), partner):
        pl.semaphore_signal(barrier, inc=1, device_id=device, device_id_type=MESH)
    for a, layer in pieces:
        prepare(a, layer).start()
    for a, layer in pieces:
        load(a, 0, layer).start()
    pl.semaphore_wait(barrier, 3)
    for a in range(n):
        wait_both(stage[a], stage_sem.at[a])
        for layer in range(layers):
            first_swap(a, layer).start()
    fetch(1)

    def total(a, step, layer, i, arrived):
        t = own[a][step, layer, i].astype(jnp.float32) + pair[a][step, layer, i].astype(jnp.float32)
        if arrived is not None:
            t = t + ring[a][arrived, layer, i].astype(jnp.float32)
        return t

    def pass_on(a, step, layer, arrived):
        @pl.loop(0, own[a].shape[2])
        def _(i):
            own[a][step, layer, i] = total(a, step, layer, i, arrived).astype(jnp.bfloat16)

        hop(a, step, layer).start()

    for a, layer in pieces:
        if layer == 0:
            take_own(a, 0)
        first_swap(a, layer).wait_recv()
        pass_on(a, 0, layer, None)

    for a in range(n):
        pltpu.make_async_copy(m_in[a], new_m[a], state_sem.at[0, a]).start()
        pltpu.make_async_copy(v_in[a], new_v[a], state_sem.at[1, a]).start()
        for layer in range(layers):
            pltpu.make_async_copy(w[a].at[layer, chip, core], old_w[a].at[layer], state_sem.at[2, a]).start()

    @pl.loop(1, last)
    def _(step):
        fetch(step + 1)
        for a, layer in pieces:
            if layer == 0:
                take_own(a, step)
                take_pair(a, step)
            hop(a, step - 1, layer).wait_recv()
            pass_on(a, step, layer, step - 1)

    for a in range(n):
        wait_both(new_m[a], state_sem.at[0, a])
        wait_both(new_v[a], state_sem.at[1, a])
        wait_both(old_w[a], state_sem.at[2, a])
    for a, layer in pieces:
        if layer == 0:
            take_own(a, last)
            take_pair(a, last)
        hop(a, last - 1, layer).wait_recv()

        @pl.loop(0, own[a].shape[2])
        def _(i):
            grad = total(a, last, layer, i, last - 1).astype(jnp.bfloat16).astype(jnp.float32)
            new = adamw(old_w[a][layer, i].astype(jnp.float32), new_m[a][layer, i], new_v[a][layer, i], grad)
            new_w[a][layer, chip, core, i], new_m[a][layer, i], new_v[a][layer, i] = new

        spread(a, 0, layer).start()
        share(a, 0, layer).start()

    @pl.loop(1, last)
    def _(step):
        for a, layer in pieces:
            spread(a, step - 1, layer).wait_recv()
            spread(a, step, layer).start()
            share(a, step, layer).start()

    for a, layer in pieces:
        spread(a, last - 1, layer).wait_recv()
        share(a, last, layer).start()

    for a in range(n):
        wait_both(new_w[a], swap_send.at[a])
        wait_both(new_w[a].at[:, pl.ds(0, last)], ring_send.at[a])
    for a in range(n):
        wait_both(pair[a], share_recv.at[a])


def write(count, *refs):
    sources, targets, sem = refs[:count], refs[count:-1], refs[-1]
    copies = [pltpu.make_async_copy(source, target, sem.at[k]) for k, (source, target) in enumerate(zip(sources, targets, strict=True))]
    for copy in copies:
        copy.start()
    for copy in copies:
        copy.wait()


def solution(mesh):
    chips = mesh.shape["dp"] // CORES

    def step(*arrays):
        terms, weights, m, v = (arrays[i : i + 3] for i in (0, 3, 6, 9))
        n, layers = len(terms), weights[0].shape[0]
        tiles = [(one.shape[1] // SUBLANES, SUBLANES, one.shape[2]) for one in m]
        whole = [(layers, chips, CORES, *tile) for tile in tiles]
        state = [(layers, *tile) for tile in tiles]
        operands = [one.reshape(shape) for one, shape in zip(terms, whole, strict=True)]
        operands += [one.reshape(shape) for one, shape in zip(weights, whole, strict=True)]
        operands += [one.reshape(shape) for part in (m, v) for one, shape in zip(part, state, strict=True)]
        sems = lambda *shape: pltpu.SemaphoreType.DMA(shape)
        vmem = lambda lead, dtype: [pltpu.VMEM((*lead, *tile), dtype) for tile in tiles]
        out = pl.pallas_call(
            functools.partial(kernel, n, chips, layers),
            out_shape=[pltpu.VMEM(shape, jnp.bfloat16) for shape in whole] + [pltpu.VMEM(shape, jnp.float32) for shape in state] * 2,
            in_specs=[pl.BlockSpec(memory_space=pl.ANY)] * len(operands),
            out_specs=[pl.BlockSpec(memory_space=pltpu.VMEM)] * (3 * n),
            scratch_shapes=[
                *vmem((chips, layers), jnp.bfloat16),
                *vmem((chips, layers), jnp.bfloat16),
                *vmem((chips - 1, layers), jnp.bfloat16),
                *vmem((layers,), jnp.bfloat16),
                *vmem((layers,), jnp.bfloat16),
                sems(n, 2),
                sems(n),
                sems(3, n),
                sems(n, layers),
                sems(n, chips - 1),
                sems(n, chips, layers),
                sems(n),
                sems(n),
                sems(n),
            ],
            compiler_params=pltpu.CompilerParams(collective_id=0, has_side_effects=True, vmem_limit_bytes=40 << 20),
            name="step",
        )(*operands)
        out = pl.pallas_call(
            functools.partial(write, len(out)),
            out_shape=[jax.ShapeDtypeStruct(one.shape, one.dtype) for one in out],
            in_specs=[pl.BlockSpec(memory_space=pltpu.VMEM)] * len(out),
            out_specs=[pl.BlockSpec(memory_space=pl.ANY)] * len(out),
            scratch_shapes=[sems(len(out))],
            compiler_params=pltpu.CompilerParams(vmem_limit_bytes=1 << 20),
            name="write",
        )(*[pltpu.with_memory_space_constraint(one, pltpu.VMEM) for one in out])
        return tuple(one.reshape(like.shape) for one, like in zip(out, (*weights, *m, *v), strict=True))

    all_of, cut = P(None, None, None), P(None, "dp", None)
    return jax.shard_map(
        step,
        mesh=mesh,
        in_specs=(P(("rep", "dp"), None, None, None),) * 3 + (all_of,) * 3 + (cut,) * 6,
        out_specs=(P("rep", None, None),) * 3 + (P("rep", "dp", None),) * 6,
        check_vma=False,
    )
```

```python
import functools

import jax
import jax.numpy as jnp
from jax import lax
from jax.experimental import pallas as pl
from jax.experimental.pallas import tpu as pltpu
from jax.sharding import PartitionSpec as P

MESH = pl.DeviceIdType.MESH
CORES = 2
SUBLANES = 8
HEAD = 1
PARTS = 4
DETOUR = 0
SLOTS = 3


def adamw(w, m, v, g):
    m = 0.9 * m + 0.1 * g
    v = 0.95 * v + 0.05 * g * g
    step = m * lax.rsqrt(v + 1e-8) + 0.1 * w
    return (w - 0.02 * step).astype(jnp.bfloat16), m, v


def cuts(count, parts):
    edges = [count * i // parts for i in range(parts + 1)]
    return [(lo, hi - lo) for lo, hi in zip(edges, edges[1:])]


def kernel(n, chips, layers, *refs):
    refs = iter(refs)
    take = lambda count: [next(refs) for _ in range(count)]
    g, w, m_in, v_in = take(n), take(n), take(n), take(n)
    new_w, new_m, new_v = take(n), take(n), take(n)
    own, pair, ring, stage, old_w = take(n), take(n), take(n), take(n), take(n)
    stage_sem, first_load, load_sem, first_recv, pair_recv, ring_recv, tail_recv, detour_recv, share_recv, swap_send, ring_send, credit = take(12)

    me = lax.axis_index("dp")
    chip, core = me // CORES, me % CORES
    other = 1 - core
    last = chips - 1
    partner = {"dp": chip * CORES + other}
    right = {"dp": (chip + 1) % chips * CORES + core}
    left = {"dp": (chip + last) % chips * CORES + core}
    ahead = [left if layer % 2 else right for layer in range(layers)]
    behind = [right if layer % 2 else left for layer in range(layers)]
    slabs = [one.shape[2] for one in own]
    pieces = [(a, layer) for a in range(n) for layer in range(layers)]
    units = [(0, 0, HEAD), (0, HEAD, slabs[0] - HEAD)] + [(a, 0, slabs[a]) for a in range(1, n)]

    def block(step, layer):
        return (chip + 1 + step if layer % 2 else chip + chips - 1 - step) % chips

    def source(step, layer):
        return (chip + step if layer % 2 else chip + chips - step) % chips

    def prepare(u, layer):
        a, lo, size = units[u]
        return pltpu.make_async_copy(
            g[a].at[layer, block(0, layer), other, pl.ds(lo, size)], stage[a].at[layer, pl.ds(lo, size)], stage_sem.at[u]
        )

    def first_own(u, layer):
        a, lo, size = units[u]
        return pltpu.make_async_copy(
            g[a].at[layer, block(0, layer), core, pl.ds(lo, size)], own[a].at[0, layer, pl.ds(lo, size)], first_load.at[u]
        )

    def first_swap(u, layer):
        a, lo, size = units[u]
        return pltpu.make_async_remote_copy(
            stage[a].at[layer, pl.ds(lo, size)], pair[a].at[0, layer, pl.ds(lo, size)], swap_send.at[a], first_recv.at[u, layer], partner, MESH
        )

    def load(a, step, layer):
        return pltpu.make_async_copy(g[a].at[layer, block(step, layer), core], own[a].at[step, layer], load_sem.at[a])

    def swap(a, step, layer, sem):
        return pltpu.make_async_remote_copy(
            g[a].at[layer, block(step, layer), other], pair[a].at[step, layer], swap_send.at[a], pair_recv.at[sem, a], partner, MESH
        )

    def hop(a, step, layer, lo=0, size=None):
        part = pl.ds(lo, slabs[a] if size is None else size)
        return pltpu.make_async_remote_copy(
            own[a].at[step, layer, part],
            ring[a].at[step, layer, part],
            ring_send.at[a],
            ring_recv.at[a, step % SLOTS, layer],
            ahead[layer],
            MESH,
        )

    def spread(a, step, layer):
        here = new_w[a].at[layer, source(step, layer), core]
        return pltpu.make_async_remote_copy(
            here, here, ring_send.at[a], ring_recv.at[a, (step + last) % SLOTS, layer], ahead[layer], MESH
        )

    def tail(layer):
        return cuts(slabs[n - 1] - (0 if layer % 2 else DETOUR), PARTS)

    def spread_tail(step, layer, k):
        here = new_w[n - 1].at[layer, source(step, layer), core, pl.ds(*tail(layer)[k])]
        return pltpu.make_async_remote_copy(here, here, ring_send.at[n - 1], tail_recv.at[k, layer], ahead[layer], MESH)

    def detour(step, layer):
        here = new_w[n - 1].at[layer, source(step, layer), core, pl.ds(slabs[n - 1] - DETOUR, DETOUR)]
        return pltpu.make_async_remote_copy(here, here, ring_send.at[n - 1], detour_recv.at[layer], behind[layer], MESH)

    def share(a, step, layer, lo=0, size=None):
        here = new_w[a].at[layer, source(step, layer), core, pl.ds(lo, slabs[a] if size is None else size)]
        return pltpu.make_async_remote_copy(here, here, swap_send.at[a], share_recv.at[a], partner, MESH)

    def wait_all(here, sem):
        pltpu.make_async_copy(here, here, sem).wait()

    def grant(layer):
        pl.semaphore_signal(credit.at[layer], inc=1, device_id=behind[layer], device_id_type=MESH)

    def spend(layer):
        pl.semaphore_wait(credit.at[layer], 1)

    for layer in range(layers):
        prepare(0, layer).start()
    for layer in range(layers):
        first_own(0, layer).start()
    barrier = pltpu.get_barrier_semaphore()
    for device in (right, left, partner):
        pl.semaphore_signal(barrier, inc=1, device_id=device, device_id_type=MESH)
    for u in range(1, n + 1):
        for layer in range(layers):
            prepare(u, layer).start()
    pl.semaphore_wait(barrier, 3)
    for u, (a, lo, size) in enumerate(units):
        wait_all(stage[a].at[:, pl.ds(lo, size)], stage_sem.at[u])
        for layer in range(layers):
            first_swap(u, layer).start()
        if u:
            for layer in range(layers):
                first_own(u, layer).start()
    for a, layer in pieces:
        swap(a, 1, layer, 0).start()

    def total(a, step, layer, i, arrived):
        t = own[a][step, layer, i].astype(jnp.float32) + pair[a][step, layer, i].astype(jnp.float32)
        if arrived is not None:
            t = t + ring[a][arrived, layer, i].astype(jnp.float32)
        return t

    def pass_on(a, step, layer, arrived, lo, size):
        @pl.loop(lo, lo + size)
        def _(i):
            own[a][step, layer, i] = total(a, step, layer, i, arrived).astype(jnp.bfloat16)

        hop(a, step, layer, lo, size).start()

    for u, (a, lo, size) in enumerate(units):
        wait_all(own[a].at[0, :, pl.ds(lo, size)], first_load.at[u])
        for layer in range(layers):
            first_swap(u, layer).wait_recv()
            pass_on(a, 0, layer, None, lo, size)

    @pl.loop(1, chips)
    def _(step):
        for a, layer in pieces:
            load(a, step, layer).start()

    @pl.loop(2, chips)
    def _(step):
        for a, layer in pieces:
            swap(a, step, layer, 1).start()

    for a in range(n):
        pltpu.make_async_copy(m_in[a], new_m[a], load_sem.at[a]).start()
        pltpu.make_async_copy(v_in[a], new_v[a], load_sem.at[a]).start()
        for layer in range(layers):
            pltpu.make_async_copy(w[a].at[layer, chip, core], old_w[a].at[layer], load_sem.at[a]).start()
    for a in range(n):
        wait_all(new_w[a].at[:, pl.ds(0, (last + 1 + 4) // CORES)], load_sem.at[a])
        wait_all(pair[a].at[1], pair_recv.at[0, a])

    @pl.loop(1, last)
    def _(step):
        @pl.when(step == 2)
        def _():
            for a in range(n):
                wait_all(pair[a].at[pl.ds(2, chips - 2)], pair_recv.at[1, a])

        @pl.when(step >= SLOTS)
        def _():
            for layer in range(layers):
                spend(layer)

        for a, layer in pieces:
            hop(a, step - 1, layer).wait_recv()
            pass_on(a, step, layer, step - 1, 0, slabs[a])
            if a == n - 1:
                grant(layer)

    for layer in range(layers):
        spend(layer)
    for a, layer in pieces:
        hop(a, last - 1, layer).wait_recv()

        @pl.loop(0, slabs[a])
        def _(i):
            grad = total(a, last, layer, i, last - 1).astype(jnp.bfloat16).astype(jnp.float32)
            new = adamw(old_w[a][layer, i].astype(jnp.float32), new_m[a][layer, i], new_v[a][layer, i], grad)
            new_w[a][layer, chip, core, i], new_m[a][layer, i], new_v[a][layer, i] = new

        spread(a, 0, layer).start()
        share(a, 0, layer).start()
        if a == n - 1:
            grant(layer)
            if DETOUR and layer % 2 == 0:
                detour(0, layer).start()

    @pl.loop(1, last - 1)
    def _(step):
        for layer in range(layers):
            spend(layer)
        for a, layer in pieces:
            spread(a, step - 1, layer).wait_recv()
            spread(a, step, layer).start()
            share(a, step, layer).start()
            if a == n - 1:

                @pl.when(step <= last - SLOTS)
                def _():
                    grant(layer)

    for layer in range(layers):
        spend(layer)
        if DETOUR and layer % 2 == 0:
            detour(0, layer).wait_recv()
            share(n - 1, last, layer, slabs[n - 1] - DETOUR, DETOUR).start()
    for a, layer in pieces:
        spread(a, last - 2, layer).wait_recv()
        if a < n - 1:
            spread(a, last - 1, layer).start()
        else:
            for k in range(PARTS):
                spread_tail(last - 1, layer, k).start()
        share(a, last - 1, layer).start()

    for a in range(n - 1):
        for layer in range(layers):
            spread(a, last - 1, layer).wait_recv()
            share(a, last, layer).start()
    for k in range(PARTS):
        for layer in range(layers):
            spread_tail(last, layer, k).wait_recv()
            share(n - 1, last, layer, *tail(layer)[k]).start()

    for a in range(n):
        wait_all(new_w[a], swap_send.at[a])
        wait_all(new_w[a].at[:, pl.ds(0, last)], ring_send.at[a])
    for a in range(n):
        wait_all(pair[a], share_recv.at[a])


def write(count, *refs):
    sources, targets, sem = refs[:count], refs[count:-1], refs[-1]
    copies = [pltpu.make_async_copy(source, target, sem.at[k]) for k, (source, target) in enumerate(zip(sources, targets, strict=True))]
    for copy in copies:
        copy.start()
    for copy in copies:
        copy.wait()


def solution(mesh):
    chips = mesh.shape["dp"] // CORES

    def step(*arrays):
        terms, weights, m, v = (arrays[i : i + 3] for i in (0, 3, 6, 9))
        n, layers = len(terms), weights[0].shape[0]
        tiles = [(one.shape[1] // SUBLANES, SUBLANES, one.shape[2]) for one in m]
        whole = [(layers, chips, CORES, *tile) for tile in tiles]
        state = [(layers, *tile) for tile in tiles]
        operands = [one.reshape(shape) for one, shape in zip(terms, whole, strict=True)]
        operands += [one.reshape(shape) for one, shape in zip(weights, whole, strict=True)]
        operands += [one.reshape(shape) for part in (m, v) for one, shape in zip(part, state, strict=True)]
        sems = lambda *shape: pltpu.SemaphoreType.DMA(shape)
        vmem = lambda lead, dtype: [pltpu.VMEM((*lead, *tile), dtype) for tile in tiles]
        out = pl.pallas_call(
            functools.partial(kernel, n, chips, layers),
            out_shape=[pltpu.VMEM(shape, jnp.bfloat16) for shape in whole] + [pltpu.VMEM(shape, jnp.float32) for shape in state] * 2,
            in_specs=[pl.BlockSpec(memory_space=pl.ANY)] * len(operands),
            out_specs=[pl.BlockSpec(memory_space=pltpu.VMEM)] * (3 * n),
            scratch_shapes=[
                *vmem((chips, layers), jnp.bfloat16),
                *vmem((chips, layers), jnp.bfloat16),
                *vmem((chips - 1, layers), jnp.bfloat16),
                *vmem((layers,), jnp.bfloat16),
                *vmem((layers,), jnp.bfloat16),
                sems(n + 1),
                sems(n + 1),
                sems(n),
                sems(n + 1, layers),
                sems(2, n),
                sems(n, SLOTS, layers),
                sems(PARTS, layers),
                sems(layers),
                sems(n),
                sems(n),
                sems(n),
                pltpu.SemaphoreType.REGULAR((layers,)),
            ],
            compiler_params=pltpu.CompilerParams(collective_id=0, has_side_effects=True, vmem_limit_bytes=40 << 20),
            name="step",
        )(*operands)
        out = pl.pallas_call(
            functools.partial(write, len(out)),
            out_shape=[jax.ShapeDtypeStruct(one.shape, one.dtype) for one in out],
            in_specs=[pl.BlockSpec(memory_space=pltpu.VMEM)] * len(out),
            out_specs=[pl.BlockSpec(memory_space=pl.ANY)] * len(out),
            scratch_shapes=[sems(len(out))],
            compiler_params=pltpu.CompilerParams(vmem_limit_bytes=1 << 20),
            name="write",
        )(*[pltpu.with_memory_space_constraint(one, pltpu.VMEM) for one in out])
        return tuple(one.reshape(like.shape) for one, like in zip(out, (*weights, *m, *v), strict=True))

    all_of, cut = P(None, None, None), P(None, "dp", None)
    return jax.shard_map(
        step,
        mesh=mesh,
        in_specs=(P(("rep", "dp"), None, None, None),) * 3 + (all_of,) * 3 + (cut,) * 6,
        out_specs=(P("rep", None, None),) * 3 + (P("rep", "dp", None),) * 6,
        check_vma=False,
    )
```

```python
import functools

import jax
import jax.numpy as jnp
from jax import lax
from jax.experimental import pallas as pl
from jax.experimental.pallas import tpu as pltpu
from jax.sharding import PartitionSpec as P

MESH = pl.DeviceIdType.MESH
CORES = 2
SUBLANES = 8
HEAD = 1
PARTS = 4
DETOUR = 6
SLOTS = 3


def adamw(w, m, v, g):
    m = 0.9 * m + 0.1 * g
    v = 0.95 * v + 0.05 * g * g
    step = m * lax.rsqrt(v + 1e-8) + 0.1 * w
    return (w - 0.02 * step).astype(jnp.bfloat16), m, v


def cuts(count, parts):
    edges = [count * i // parts for i in range(parts + 1)]
    return [(lo, hi - lo) for lo, hi in zip(edges, edges[1:])]


def kernel(n, chips, layers, *refs):
    refs = iter(refs)
    take = lambda count: [next(refs) for _ in range(count)]
    g, w, m_in, v_in = take(n), take(n), take(n), take(n)
    new_w, new_m, new_v = take(n), take(n), take(n)
    own, pair, ring, stage, old_w = take(n), take(n), take(n), take(n), take(n)
    stage_sem, first_load, load_sem, first_recv, pair_recv, ring_recv, tail_recv, detour_recv, share_recv, swap_send, ring_send, credit = take(12)

    me = lax.axis_index("dp")
    chip, core = me // CORES, me % CORES
    other = 1 - core
    last = chips - 1
    partner = {"dp": chip * CORES + other}
    right = {"dp": (chip + 1) % chips * CORES + core}
    left = {"dp": (chip + last) % chips * CORES + core}
    ahead = [left if layer % 2 else right for layer in range(layers)]
    behind = [right if layer % 2 else left for layer in range(layers)]
    slabs = [one.shape[2] for one in own]
    pieces = [(a, layer) for a in range(n) for layer in range(layers)]
    units = [(0, 0, HEAD), (0, HEAD, slabs[0] - HEAD)] + [(a, 0, slabs[a]) for a in range(1, n)]

    def block(step, layer):
        return (chip + 1 + step if layer % 2 else chip + chips - 1 - step) % chips

    def source(step, layer):
        return (chip + step if layer % 2 else chip + chips - step) % chips

    def prepare(u, layer):
        a, lo, size = units[u]
        return pltpu.make_async_copy(
            g[a].at[layer, block(0, layer), other, pl.ds(lo, size)], stage[a].at[layer, pl.ds(lo, size)], stage_sem.at[u]
        )

    def first_own(u, layer):
        a, lo, size = units[u]
        return pltpu.make_async_copy(
            g[a].at[layer, block(0, layer), core, pl.ds(lo, size)], own[a].at[0, layer, pl.ds(lo, size)], first_load.at[u]
        )

    def first_swap(u, layer):
        a, lo, size = units[u]
        return pltpu.make_async_remote_copy(
            stage[a].at[layer, pl.ds(lo, size)], pair[a].at[0, layer, pl.ds(lo, size)], swap_send.at[a], first_recv.at[u, layer], partner, MESH
        )

    def load(a, step, layer):
        return pltpu.make_async_copy(g[a].at[layer, block(step, layer), core], own[a].at[step, layer], load_sem.at[a])

    def swap(a, step, layer, sem):
        return pltpu.make_async_remote_copy(
            g[a].at[layer, block(step, layer), other], pair[a].at[step, layer], swap_send.at[a], pair_recv.at[sem, a], partner, MESH
        )

    def hop(a, step, layer, lo=0, size=None):
        part = pl.ds(lo, slabs[a] if size is None else size)
        return pltpu.make_async_remote_copy(
            own[a].at[step, layer, part],
            ring[a].at[step, layer, part],
            ring_send.at[a],
            ring_recv.at[a, step % SLOTS, layer],
            ahead[layer],
            MESH,
        )

    def spread(a, step, layer):
        here = new_w[a].at[layer, source(step, layer), core]
        return pltpu.make_async_remote_copy(
            here, here, ring_send.at[a], ring_recv.at[a, (step + last) % SLOTS, layer], ahead[layer], MESH
        )

    def tail(layer):
        return cuts(slabs[n - 1] - (0 if layer % 2 else DETOUR), PARTS)

    def spread_tail(step, layer, k):
        here = new_w[n - 1].at[layer, source(step, layer), core, pl.ds(*tail(layer)[k])]
        return pltpu.make_async_remote_copy(here, here, ring_send.at[n - 1], tail_recv.at[k, layer], ahead[layer], MESH)

    def detour(step, layer):
        here = new_w[n - 1].at[layer, source(step, layer), core, pl.ds(slabs[n - 1] - DETOUR, DETOUR)]
        return pltpu.make_async_remote_copy(here, here, ring_send.at[n - 1], detour_recv.at[layer], behind[layer], MESH)

    def share(a, step, layer, lo=0, size=None):
        here = new_w[a].at[layer, source(step, layer), core, pl.ds(lo, slabs[a] if size is None else size)]
        return pltpu.make_async_remote_copy(here, here, swap_send.at[a], share_recv.at[a], partner, MESH)

    def wait_all(here, sem):
        pltpu.make_async_copy(here, here, sem).wait()

    def grant(layer):
        pl.semaphore_signal(credit.at[layer], inc=1, device_id=behind[layer], device_id_type=MESH)

    def spend(layer):
        pl.semaphore_wait(credit.at[layer], 1)

    for layer in range(layers):
        prepare(0, layer).start()
    for layer in range(layers):
        first_own(0, layer).start()
    barrier = pltpu.get_barrier_semaphore()
    for device in (right, left, partner):
        pl.semaphore_signal(barrier, inc=1, device_id=device, device_id_type=MESH)
    for u in range(1, n + 1):
        for layer in range(layers):
            prepare(u, layer).start()
    pl.semaphore_wait(barrier, 3)
    for u, (a, lo, size) in enumerate(units):
        wait_all(stage[a].at[:, pl.ds(lo, size)], stage_sem.at[u])
        for layer in range(layers):
            first_swap(u, layer).start()
        if u:
            for layer in range(layers):
                first_own(u, layer).start()
    for a, layer in pieces:
        swap(a, 1, layer, 0).start()

    def total(a, step, layer, i, arrived):
        t = own[a][step, layer, i].astype(jnp.float32) + pair[a][step, layer, i].astype(jnp.float32)
        if arrived is not None:
            t = t + ring[a][arrived, layer, i].astype(jnp.float32)
        return t

    def pass_on(a, step, layer, arrived, lo, size):
        @pl.loop(lo, lo + size)
        def _(i):
            own[a][step, layer, i] = total(a, step, layer, i, arrived).astype(jnp.bfloat16)

        hop(a, step, layer, lo, size).start()

    for u, (a, lo, size) in enumerate(units):
        wait_all(own[a].at[0, :, pl.ds(lo, size)], first_load.at[u])
        for layer in range(layers):
            first_swap(u, layer).wait_recv()
            pass_on(a, 0, layer, None, lo, size)

    @pl.loop(1, chips)
    def _(step):
        for a, layer in pieces:
            load(a, step, layer).start()

    @pl.loop(2, chips)
    def _(step):
        for a, layer in pieces:
            swap(a, step, layer, 1).start()

    for a in range(n):
        pltpu.make_async_copy(m_in[a], new_m[a], load_sem.at[a]).start()
        pltpu.make_async_copy(v_in[a], new_v[a], load_sem.at[a]).start()
        for layer in range(layers):
            pltpu.make_async_copy(w[a].at[layer, chip, core], old_w[a].at[layer], load_sem.at[a]).start()
    for a in range(n):
        wait_all(new_w[a].at[:, pl.ds(0, (last + 1 + 4) // CORES)], load_sem.at[a])
        wait_all(pair[a].at[1], pair_recv.at[0, a])

    @pl.loop(1, last)
    def _(step):
        @pl.when(step == 2)
        def _():
            for a in range(n):
                wait_all(pair[a].at[pl.ds(2, chips - 2)], pair_recv.at[1, a])

        @pl.when(step >= SLOTS)
        def _():
            for layer in range(layers):
                spend(layer)

        for a, layer in pieces:
            hop(a, step - 1, layer).wait_recv()
            pass_on(a, step, layer, step - 1, 0, slabs[a])
            if a == n - 1:
                grant(layer)

    for layer in range(layers):
        spend(layer)
    for a, layer in pieces:
        hop(a, last - 1, layer).wait_recv()

        @pl.loop(0, slabs[a])
        def _(i):
            grad = total(a, last, layer, i, last - 1).astype(jnp.bfloat16).astype(jnp.float32)
            new = adamw(old_w[a][layer, i].astype(jnp.float32), new_m[a][layer, i], new_v[a][layer, i], grad)
            new_w[a][layer, chip, core, i], new_m[a][layer, i], new_v[a][layer, i] = new

        spread(a, 0, layer).start()
        share(a, 0, layer).start()
        if a == n - 1:
            grant(layer)
            if DETOUR and layer % 2 == 0:
                detour(0, layer).start()

    @pl.loop(1, last - 1)
    def _(step):
        for layer in range(layers):
            spend(layer)
        for a, layer in pieces:
            spread(a, step - 1, layer).wait_recv()
            spread(a, step, layer).start()
            share(a, step, layer).start()
            if a == n - 1:

                @pl.when(step <= last - SLOTS)
                def _():
                    grant(layer)

    for layer in range(layers):
        spend(layer)
        if DETOUR and layer % 2 == 0:
            detour(0, layer).wait_recv()
            share(n - 1, last, layer, slabs[n - 1] - DETOUR, DETOUR).start()
    for a, layer in pieces:
        spread(a, last - 2, layer).wait_recv()
        if a < n - 1:
            spread(a, last - 1, layer).start()
        else:
            for k in range(PARTS):
                spread_tail(last - 1, layer, k).start()
        share(a, last - 1, layer).start()

    for a in range(n - 1):
        for layer in range(layers):
            spread(a, last - 1, layer).wait_recv()
            share(a, last, layer).start()
    for k in range(PARTS):
        for layer in range(layers):
            spread_tail(last, layer, k).wait_recv()
            share(n - 1, last, layer, *tail(layer)[k]).start()

    for a in range(n):
        wait_all(new_w[a], swap_send.at[a])
        wait_all(new_w[a].at[:, pl.ds(0, last)], ring_send.at[a])
    for a in range(n):
        wait_all(pair[a], share_recv.at[a])


def write(n, *refs):
    *refs, sem = refs
    sources, targets = refs[: 3 * n], refs[3 * n :]
    copies = [
        pltpu.make_async_copy(source, target, sem.at[min(k, n)]) for k, (source, target) in enumerate(zip(sources, targets, strict=True))
    ]
    for copy in copies:
        copy.start()
    for copy in copies[:n]:
        copy.wait()
    part = sources[0].at[:, pl.ds(0, 2 * n)]
    pltpu.make_async_copy(part, part, sem.at[n]).wait()


def solution(mesh):
    chips = mesh.shape["dp"] // CORES

    def step(*arrays):
        terms, weights, m, v = (arrays[i : i + 3] for i in (0, 3, 6, 9))
        n, layers = len(terms), weights[0].shape[0]
        tiles = [(one.shape[1] // SUBLANES, SUBLANES, one.shape[2]) for one in m]
        whole = [(layers, chips, CORES, *tile) for tile in tiles]
        state = [(layers, *tile) for tile in tiles]
        operands = [one.reshape(shape) for one, shape in zip(terms, whole, strict=True)]
        operands += [one.reshape(shape) for one, shape in zip(weights, whole, strict=True)]
        operands += [one.reshape(shape) for part in (m, v) for one, shape in zip(part, state, strict=True)]
        sems = lambda *shape: pltpu.SemaphoreType.DMA(shape)
        vmem = lambda lead, dtype: [pltpu.VMEM((*lead, *tile), dtype) for tile in tiles]
        out = pl.pallas_call(
            functools.partial(kernel, n, chips, layers),
            out_shape=[pltpu.VMEM(shape, jnp.bfloat16) for shape in whole] + [pltpu.VMEM(shape, jnp.float32) for shape in state] * 2,
            in_specs=[pl.BlockSpec(memory_space=pl.ANY)] * len(operands),
            out_specs=[pl.BlockSpec(memory_space=pltpu.VMEM)] * (3 * n),
            scratch_shapes=[
                *vmem((chips, layers), jnp.bfloat16),
                *vmem((chips, layers), jnp.bfloat16),
                *vmem((chips - 1, layers), jnp.bfloat16),
                *vmem((layers,), jnp.bfloat16),
                *vmem((layers,), jnp.bfloat16),
                sems(n + 1),
                sems(n + 1),
                sems(n),
                sems(n + 1, layers),
                sems(2, n),
                sems(n, SLOTS, layers),
                sems(PARTS, layers),
                sems(layers),
                sems(n),
                sems(n),
                sems(n),
                pltpu.SemaphoreType.REGULAR((layers,)),
            ],
            compiler_params=pltpu.CompilerParams(collective_id=0, has_side_effects=True, vmem_limit_bytes=40 << 20),
            name="step",
        )(*operands)
        out = pl.pallas_call(
            functools.partial(write, n),
            out_shape=[jax.ShapeDtypeStruct(one.shape, one.dtype) for one in out],
            in_specs=[pl.BlockSpec(memory_space=pltpu.VMEM)] * len(out),
            out_specs=[pl.BlockSpec(memory_space=pl.ANY)] * len(out),
            scratch_shapes=[sems(n + 1)],
            compiler_params=pltpu.CompilerParams(vmem_limit_bytes=1 << 20),
            name="write",
        )(*[pltpu.with_memory_space_constraint(one, pltpu.VMEM) for one in out])
        return tuple(one.reshape(like.shape) for one, like in zip(out, (*weights, *m, *v), strict=True))

    all_of, cut = P(None, None, None), P(None, "dp", None)
    return jax.shard_map(
        step,
        mesh=mesh,
        in_specs=(P(("rep", "dp"), None, None, None),) * 3 + (all_of,) * 3 + (cut,) * 6,
        out_specs=(P("rep", None, None),) * 3 + (P("rep", "dp", None),) * 6,
        check_vma=False,
    )
```

```python
import functools

import jax
import jax.numpy as jnp
from jax import lax
from jax.experimental import pallas as pl
from jax.experimental.pallas import tpu as pltpu
from jax.sharding import PartitionSpec as P

MESH = pl.DeviceIdType.MESH
CORES = 2
SUBLANES = 8
HEAD = 1
PARTS = 4
DETOUR = 10
SLOTS = 3


def adamw(w, m, v, g):
    m = 0.9 * m + 0.1 * g
    v = 0.95 * v + 0.05 * g * g
    step = m * lax.rsqrt(v + 1e-8) + 0.1 * w
    return (w - 0.02 * step).astype(jnp.bfloat16), m, v


def cuts(count, parts):
    edges = [count * i // parts for i in range(parts + 1)]
    return [(lo, hi - lo) for lo, hi in zip(edges, edges[1:])]


def kernel(n, chips, layers, *refs):
    refs = iter(refs)
    take = lambda count: [next(refs) for _ in range(count)]
    g, w, m_in, v_in = take(n), take(n), take(n), take(n)
    new_w, new_m, new_v = take(n), take(n), take(n)
    own, pair, ring, stage, old_w = take(n), take(n), take(n), take(n), take(n)
    stage_sem, first_load, load_sem, first_recv, pair_recv, ring_recv, tail_recv, detour_recv, share_recv, swap_send, ring_send, credit, entered = take(13)

    me = lax.axis_index("dp")
    chip, core = me // CORES, me % CORES
    other = 1 - core
    last = chips - 1
    partner = {"dp": chip * CORES + other}
    right = {"dp": (chip + 1) % chips * CORES + core}
    left = {"dp": (chip + last) % chips * CORES + core}
    ahead = [left if layer % 2 else right for layer in range(layers)]
    behind = [right if layer % 2 else left for layer in range(layers)]
    slabs = [one.shape[2] for one in own]
    pieces = [(a, layer) for a in range(n) for layer in range(layers)]
    units = [(0, 0, HEAD), (0, HEAD, slabs[0] - HEAD)] + [(a, 0, slabs[a]) for a in range(1, n)]

    def block(step, layer):
        return (chip + 1 + step if layer % 2 else chip + chips - 1 - step) % chips

    def source(step, layer):
        return (chip + step if layer % 2 else chip + chips - step) % chips

    def prepare(u, layer):
        a, lo, size = units[u]
        return pltpu.make_async_copy(
            g[a].at[layer, block(0, layer), other, pl.ds(lo, size)], stage[a].at[layer, pl.ds(lo, size)], stage_sem.at[u]
        )

    def first_own(u, layer):
        a, lo, size = units[u]
        return pltpu.make_async_copy(
            g[a].at[layer, block(0, layer), core, pl.ds(lo, size)], own[a].at[0, layer, pl.ds(lo, size)], first_load.at[u]
        )

    def first_swap(u, layer):
        a, lo, size = units[u]
        return pltpu.make_async_remote_copy(
            stage[a].at[layer, pl.ds(lo, size)], pair[a].at[0, layer, pl.ds(lo, size)], swap_send.at[a], first_recv.at[u, layer], partner, MESH
        )

    def load(a, step, layer):
        return pltpu.make_async_copy(g[a].at[layer, block(step, layer), core], own[a].at[step, layer], load_sem.at[a])

    def swap(a, step, layer, sem):
        return pltpu.make_async_remote_copy(
            g[a].at[layer, block(step, layer), other], pair[a].at[step, layer], swap_send.at[a], pair_recv.at[sem, a], partner, MESH
        )

    def hop(a, step, layer, lo=0, size=None):
        part = pl.ds(lo, slabs[a] if size is None else size)
        return pltpu.make_async_remote_copy(
            own[a].at[step, layer, part],
            ring[a].at[step, layer, part],
            ring_send.at[a],
            ring_recv.at[a, step % SLOTS, layer],
            ahead[layer],
            MESH,
        )

    def spread(a, step, layer):
        here = new_w[a].at[layer, source(step, layer), core]
        return pltpu.make_async_remote_copy(
            here, here, ring_send.at[a], ring_recv.at[a, (step + last) % SLOTS, layer], ahead[layer], MESH
        )

    def tail(layer):
        return cuts(slabs[n - 1] - (0 if layer % 2 else DETOUR), PARTS)

    def spread_tail(step, layer, k):
        here = new_w[n - 1].at[layer, source(step, layer), core, pl.ds(*tail(layer)[k])]
        return pltpu.make_async_remote_copy(here, here, ring_send.at[n - 1], tail_recv.at[k, layer], ahead[layer], MESH)

    def detour(step, layer):
        here = new_w[n - 1].at[layer, source(step, layer), core, pl.ds(slabs[n - 1] - DETOUR, DETOUR)]
        return pltpu.make_async_remote_copy(here, here, ring_send.at[n - 1], detour_recv.at[layer], behind[layer], MESH)

    def share(a, step, layer, lo=0, size=None):
        here = new_w[a].at[layer, source(step, layer), core, pl.ds(lo, slabs[a] if size is None else size)]
        return pltpu.make_async_remote_copy(here, here, swap_send.at[a], share_recv.at[a], partner, MESH)

    def wait_all(here, sem):
        pltpu.make_async_copy(here, here, sem).wait()

    def grant(layer):
        pl.semaphore_signal(credit.at[layer], inc=1, device_id=behind[layer], device_id_type=MESH)

    def spend(layer):
        pl.semaphore_wait(credit.at[layer], 1)

    for layer in range(layers):
        prepare(0, layer).start()
    for layer in range(layers):
        first_own(0, layer).start()
    barrier = pltpu.get_barrier_semaphore()

    def greet(device):
        pl.semaphore_signal(barrier, inc=1, device_id=device, device_id_type=MESH)

    def answer(which, device):
        pl.semaphore_signal(entered.at[which], inc=1, device_id=device, device_id_type=MESH)

    def answer_chips():
        @pl.when(chip > 0)
        def _():
            answer(0, left)

        @pl.when(chip == last)
        def _():
            answer(1, right)

    greeted = jnp.where(chip > 0, 1, 0) + jnp.where(chip == last, 1, 0)
    pl.when(chip < last)(lambda: greet(right))
    pl.when(chip == 0)(lambda: greet(left))
    pl.when(core == 0)(lambda: greet(partner))
    for u in range(1, n + 1):
        for layer in range(layers):
            prepare(u, layer).start()

    @pl.when(core > 0)
    def _():
        pl.semaphore_wait(barrier, greeted + 1)
        answer(2, partner)
        answer_chips()

    @pl.when(core == 0)
    def _():
        pl.semaphore_wait(entered.at[2], 1)

    for u, (a, lo, size) in enumerate(units):
        wait_all(stage[a].at[:, pl.ds(lo, size)], stage_sem.at[u])
        for layer in range(layers):
            first_swap(u, layer).start()
        if u:
            for layer in range(layers):
                first_own(u, layer).start()
    for a, layer in pieces:
        swap(a, 1, layer, 0).start()

    @pl.when(core == 0)
    def _():
        @pl.when(chip > 0)
        def _():
            pl.semaphore_wait(barrier, greeted)

        answer_chips()

    def total(a, step, layer, i, arrived):
        t = own[a][step, layer, i].astype(jnp.float32) + pair[a][step, layer, i].astype(jnp.float32)
        if arrived is not None:
            t = t + ring[a][arrived, layer, i].astype(jnp.float32)
        return t

    def add(a, step, layer, arrived, lo, size):
        @pl.loop(lo, lo + size)
        def _(i):
            own[a][step, layer, i] = total(a, step, layer, i, arrived).astype(jnp.bfloat16)

    for u, (a, lo, size) in enumerate(units):
        wait_all(own[a].at[0, :, pl.ds(lo, size)], first_load.at[u])
        for layer in range(layers):
            first_swap(u, layer).wait_recv()
            add(a, 0, layer, None, lo, size)
        for layer in reversed(range(layers)):
            if u == 0 and layer < 2:

                @pl.when(chip == 0 if layer else chip < last)
                def _():
                    pl.semaphore_wait(entered.at[layer], 1)

            hop(a, 0, layer, lo, size).start()

    @pl.loop(1, chips)
    def _(step):
        for a, layer in pieces:
            load(a, step, layer).start()

    @pl.loop(2, chips)
    def _(step):
        for a, layer in pieces:
            swap(a, step, layer, 1).start()

    for a in range(n):
        pltpu.make_async_copy(m_in[a], new_m[a], load_sem.at[a]).start()
        pltpu.make_async_copy(v_in[a], new_v[a], load_sem.at[a]).start()
        for layer in range(layers):
            pltpu.make_async_copy(w[a].at[layer, chip, core], old_w[a].at[layer], load_sem.at[a]).start()
    for a in range(n):
        wait_all(new_w[a].at[:, pl.ds(0, (last + 1 + 4) // CORES)], load_sem.at[a])
        wait_all(pair[a].at[1], pair_recv.at[0, a])

    @pl.loop(1, last)
    def _(step):
        @pl.when(step == 2)
        def _():
            for a in range(n):
                wait_all(pair[a].at[pl.ds(2, chips - 2)], pair_recv.at[1, a])

        @pl.when(step >= SLOTS)
        def _():
            for layer in range(layers):
                spend(layer)

        for a, layer in pieces:
            hop(a, step - 1, layer).wait_recv()
            add(a, step, layer, step - 1, 0, slabs[a])
            hop(a, step, layer).start()
            if a == n - 1:
                grant(layer)

    for layer in range(layers):
        spend(layer)
    for a, layer in pieces:
        hop(a, last - 1, layer).wait_recv()

        @pl.loop(0, slabs[a])
        def _(i):
            grad = total(a, last, layer, i, last - 1).astype(jnp.bfloat16).astype(jnp.float32)
            new = adamw(old_w[a][layer, i].astype(jnp.float32), new_m[a][layer, i], new_v[a][layer, i], grad)
            new_w[a][layer, chip, core, i], new_m[a][layer, i], new_v[a][layer, i] = new

        spread(a, 0, layer).start()
        share(a, 0, layer).start()
        if a == n - 1:
            grant(layer)
            if DETOUR and layer % 2 == 0:
                detour(0, layer).start()

    @pl.loop(1, last - 1)
    def _(step):
        for layer in range(layers):
            spend(layer)
        for a, layer in pieces:
            spread(a, step - 1, layer).wait_recv()
            spread(a, step, layer).start()
            share(a, step, layer).start()
            if a == n - 1:

                @pl.when(step <= last - SLOTS)
                def _():
                    grant(layer)

    for layer in range(layers):
        spend(layer)
        if DETOUR and layer % 2 == 0:
            detour(0, layer).wait_recv()
            share(n - 1, last, layer, slabs[n - 1] - DETOUR, DETOUR).start()
    for a, layer in pieces:
        spread(a, last - 2, layer).wait_recv()
        if a < n - 1:
            spread(a, last - 1, layer).start()
        else:
            for k in range(PARTS):
                spread_tail(last - 1, layer, k).start()
        share(a, last - 1, layer).start()

    for a in range(n - 1):
        for layer in range(layers):
            spread(a, last - 1, layer).wait_recv()
            share(a, last, layer).start()
    for k in range(PARTS):
        for layer in range(layers):
            spread_tail(last, layer, k).wait_recv()
            share(n - 1, last, layer, *tail(layer)[k]).start()

    for a in range(n):
        wait_all(new_w[a], swap_send.at[a])
        wait_all(new_w[a].at[:, pl.ds(0, last)], ring_send.at[a])
    for a in range(n):
        wait_all(pair[a], share_recv.at[a])


def write(n, *refs):
    *refs, sem = refs
    sources, targets = refs[: 3 * n], refs[3 * n :]
    copies = [
        pltpu.make_async_copy(source, target, sem.at[min(k, n)]) for k, (source, target) in enumerate(zip(sources, targets, strict=True))
    ]
    for copy in copies:
        copy.start()
    for copy in copies[:n]:
        copy.wait()
    part = sources[0].at[:, pl.ds(0, 2 * n)]
    pltpu.make_async_copy(part, part, sem.at[n]).wait()


def solution(mesh):
    chips = mesh.shape["dp"] // CORES

    def step(*arrays):
        terms, weights, m, v = (arrays[i : i + 3] for i in (0, 3, 6, 9))
        n, layers = len(terms), weights[0].shape[0]
        tiles = [(one.shape[1] // SUBLANES, SUBLANES, one.shape[2]) for one in m]
        whole = [(layers, chips, CORES, *tile) for tile in tiles]
        state = [(layers, *tile) for tile in tiles]
        operands = [one.reshape(shape) for one, shape in zip(terms, whole, strict=True)]
        operands += [one.reshape(shape) for one, shape in zip(weights, whole, strict=True)]
        operands += [one.reshape(shape) for part in (m, v) for one, shape in zip(part, state, strict=True)]
        sems = lambda *shape: pltpu.SemaphoreType.DMA(shape)
        vmem = lambda lead, dtype: [pltpu.VMEM((*lead, *tile), dtype) for tile in tiles]
        out = pl.pallas_call(
            functools.partial(kernel, n, chips, layers),
            out_shape=[pltpu.VMEM(shape, jnp.bfloat16) for shape in whole] + [pltpu.VMEM(shape, jnp.float32) for shape in state] * 2,
            in_specs=[pl.BlockSpec(memory_space=pl.ANY)] * len(operands),
            out_specs=[pl.BlockSpec(memory_space=pltpu.VMEM)] * (3 * n),
            scratch_shapes=[
                *vmem((chips, layers), jnp.bfloat16),
                *vmem((chips, layers), jnp.bfloat16),
                *vmem((chips - 1, layers), jnp.bfloat16),
                *vmem((layers,), jnp.bfloat16),
                *vmem((layers,), jnp.bfloat16),
                sems(n + 1),
                sems(n + 1),
                sems(n),
                sems(n + 1, layers),
                sems(2, n),
                sems(n, SLOTS, layers),
                sems(PARTS, layers),
                sems(layers),
                sems(n),
                sems(n),
                sems(n),
                pltpu.SemaphoreType.REGULAR((layers,)),
                pltpu.SemaphoreType.REGULAR((3,)),
            ],
            compiler_params=pltpu.CompilerParams(collective_id=0, has_side_effects=True, vmem_limit_bytes=40 << 20),
            name="step",
        )(*operands)
        out = pl.pallas_call(
            functools.partial(write, n),
            out_shape=[jax.ShapeDtypeStruct(one.shape, one.dtype) for one in out],
            in_specs=[pl.BlockSpec(memory_space=pltpu.VMEM)] * len(out),
            out_specs=[pl.BlockSpec(memory_space=pl.ANY)] * len(out),
            scratch_shapes=[sems(n + 1)],
            compiler_params=pltpu.CompilerParams(vmem_limit_bytes=1 << 20),
            name="write",
        )(*[pltpu.with_memory_space_constraint(one, pltpu.VMEM) for one in out])
        return tuple(one.reshape(like.shape) for one, like in zip(out, (*weights, *m, *v), strict=True))

    all_of, cut = P(None, None, None), P(None, "dp", None)
    return jax.shard_map(
        step,
        mesh=mesh,
        in_specs=(P(("rep", "dp"), None, None, None),) * 3 + (all_of,) * 3 + (cut,) * 6,
        out_specs=(P("rep", None, None),) * 3 + (P("rep", "dp", None),) * 6,
        check_vma=False,
    )
```

```python
import functools

import jax
import jax.numpy as jnp
from jax import lax
from jax.experimental import pallas as pl
from jax.experimental.pallas import tpu as pltpu
from jax.sharding import PartitionSpec as P

MESH = pl.DeviceIdType.MESH
CORES = 2
SUBLANES = 8
HEAD = 1
PARTS = 4
SEAM = 13
DETOUR = 5
SLOTS = 3


def adamw(w, m, v, g):
    m = 0.9 * m + 0.1 * g
    v = 0.95 * v + 0.05 * g * g
    step = m * lax.rsqrt(v + 1e-8) + 0.1 * w
    return (w - 0.02 * step).astype(jnp.bfloat16), m, v


def cuts(count, parts):
    edges = [count * i // parts for i in range(parts + 1)]
    return [(lo, hi - lo) for lo, hi in zip(edges, edges[1:])]


def kernel(n, chips, layers, *refs):
    refs = iter(refs)
    take = lambda count: [next(refs) for _ in range(count)]
    g, w, m_in, v_in = take(n), take(n), take(n), take(n)
    new_w, new_m, new_v = take(n), take(n), take(n)
    own, pair, ring, stage, old_w, (extra,) = take(n), take(n), take(n), take(n), take(n), take(1)
    stage_sem, first_load, load_sem, first_recv, pair_recv, ring_recv, tail_recv, extra_recv, share_recv, swap_send, ring_send, gather_send, tail_send, credit, entered = take(15)

    me = lax.axis_index("dp")
    chip, core = me // CORES, me % CORES
    other = 1 - core
    last = chips - 1
    partner = {"dp": chip * CORES + other}
    right = {"dp": (chip + 1) % chips * CORES + core}
    left = {"dp": (chip + last) % chips * CORES + core}
    ahead = [left if layer % 2 else right for layer in range(layers)]
    behind = [right if layer % 2 else left for layer in range(layers)]
    slabs = [one.shape[2] for one in own]
    end = n - 1
    whole, split = slabs[end], slabs[end] - SEAM
    pieces = [(a, layer) for a in range(n) for layer in range(layers)]
    units = [(0, 0, HEAD), (0, HEAD, slabs[0] - HEAD)] + [(a, 0, slabs[a]) for a in range(1, n)]

    def block(step, layer):
        return (chip + 1 + step if layer % 2 else chip + chips - 1 - step) % chips

    def source(step, layer):
        return (chip + step if layer % 2 else chip + chips - step) % chips

    def prepare(u, layer):
        a, lo, size = units[u]
        return pltpu.make_async_copy(
            g[a].at[layer, block(0, layer), other, pl.ds(lo, size)], stage[a].at[layer, pl.ds(lo, size)], stage_sem.at[u]
        )

    def first_own(u, layer):
        a, lo, size = units[u]
        return pltpu.make_async_copy(
            g[a].at[layer, block(0, layer), core, pl.ds(lo, size)], own[a].at[0, layer, pl.ds(lo, size)], first_load.at[u]
        )

    def first_swap(u, layer):
        a, lo, size = units[u]
        return pltpu.make_async_remote_copy(
            stage[a].at[layer, pl.ds(lo, size)], pair[a].at[0, layer, pl.ds(lo, size)], swap_send.at[a], first_recv.at[u, layer], partner, MESH
        )

    def load(a, step, layer):
        return pltpu.make_async_copy(g[a].at[layer, block(step, layer), core], own[a].at[step, layer], load_sem.at[a])

    def swap(a, step, layer, sem):
        return pltpu.make_async_remote_copy(
            g[a].at[layer, block(step, layer), other], pair[a].at[step, layer], swap_send.at[a], pair_recv.at[sem, a], partner, MESH
        )

    def hop(a, step, layer, lo=0, size=None):
        part = pl.ds(lo, slabs[a] if size is None else size)
        return pltpu.make_async_remote_copy(
            own[a].at[step, layer, part],
            ring[a].at[step, layer, part],
            ring_send.at[a],
            ring_recv.at[a, step % SLOTS, layer],
            ahead[layer],
            MESH,
        )

    def spread(a, step, layer):
        here = new_w[a].at[layer, source(step, layer), core]
        return pltpu.make_async_remote_copy(
            here, here, gather_send.at[a], ring_recv.at[a, (step + last) % SLOTS, layer], ahead[layer], MESH
        )

    def straight():
        return pltpu.make_async_remote_copy(own[end].at[0, 0, pl.ds(split, SEAM)], extra, ring_send.at[end], extra_recv, left, MESH)

    tail = [cuts(whole, PARTS) if layer else [(whole - DETOUR, DETOUR), *cuts(whole - DETOUR, PARTS)] for layer in range(layers)]

    def spread_tail(step, layer, k):
        here = new_w[end].at[layer, source(step, layer), core, pl.ds(*tail[layer][k])]
        sem = tail_send.at[layers if layer == k == 0 else layer]
        return pltpu.make_async_remote_copy(here, here, sem, tail_recv.at[k, layer], ahead[layer], MESH)

    def detour(step):
        here = new_w[end].at[0, source(step, 0), core, pl.ds(*tail[0][0])]
        return pltpu.make_async_remote_copy(here, here, tail_send.at[layers + 1], tail_recv.at[0, 0], left, MESH)

    def share(a, step, layer, lo=0, size=None):
        here = new_w[a].at[layer, source(step, layer), core, pl.ds(lo, slabs[a] if size is None else size)]
        return pltpu.make_async_remote_copy(here, here, swap_send.at[a], share_recv.at[a], partner, MESH)

    def wait_all(here, sem):
        pltpu.make_async_copy(here, here, sem).wait()

    def grant(layer):
        pl.semaphore_signal(credit.at[layer], inc=1, device_id=behind[layer], device_id_type=MESH)

    def spend(layer):
        pl.semaphore_wait(credit.at[layer], 1)

    for layer in range(layers):
        prepare(0, layer).start()
    for layer in range(layers):
        first_own(0, layer).start()
    barrier = pltpu.get_barrier_semaphore()

    def greet(device):
        pl.semaphore_signal(barrier, inc=1, device_id=device, device_id_type=MESH)

    def answer(which, device):
        pl.semaphore_signal(entered.at[which], inc=1, device_id=device, device_id_type=MESH)

    def answer_chips():
        @pl.when(chip > 0)
        def _():
            answer(0, left)

        @pl.when(chip == last)
        def _():
            answer(1, right)

    greeted = jnp.where(chip > 0, 1, 0) + jnp.where(chip == last, 1, 0)
    pl.when(chip < last)(lambda: greet(right))
    pl.when(chip == 0)(lambda: greet(left))
    pl.when(core == 0)(lambda: greet(partner))
    for u in range(1, n + 1):
        for layer in range(layers):
            prepare(u, layer).start()

    @pl.when(core > 0)
    def _():
        pl.semaphore_wait(barrier, greeted + 1)
        answer(2, partner)
        answer_chips()

    @pl.when(core == 0)
    def _():
        pl.semaphore_wait(entered.at[2], 1)

    for u, (a, lo, size) in enumerate(units):
        wait_all(stage[a].at[:, pl.ds(lo, size)], stage_sem.at[u])
        for layer in range(layers):
            first_swap(u, layer).start()
        if u:
            for layer in range(layers):
                first_own(u, layer).start()
    for a, layer in pieces:
        swap(a, 1, layer, 0).start()

    @pl.when(core == 0)
    def _():
        @pl.when(chip > 0)
        def _():
            pl.semaphore_wait(barrier, greeted)

        answer_chips()

    def total(a, step, layer, i, arrived):
        t = own[a][step, layer, i].astype(jnp.float32) + pair[a][step, layer, i].astype(jnp.float32)
        if arrived is not None:
            t = t + ring[a][arrived, layer, i].astype(jnp.float32)
        return t

    def add(a, step, layer, arrived, lo, size):
        @pl.loop(lo, lo + size)
        def _(i):
            own[a][step, layer, i] = total(a, step, layer, i, arrived).astype(jnp.bfloat16)

    for u, (a, lo, size) in enumerate(units):
        wait_all(own[a].at[0, :, pl.ds(lo, size)], first_load.at[u])
        for layer in range(layers):
            first_swap(u, layer).wait_recv()
            add(a, 0, layer, None, lo, size)

        @pl.when(chip > 0)
        def _():
            hop(a, 0, 1, lo, size).start()

        if u == 0:

            @pl.when(chip < last)
            def _():
                pl.semaphore_wait(entered.at[0], 1)

        if a < end:
            hop(a, 0, 0, lo, size).start()
        else:
            hop(a, 0, 0, 0, split).start()

            @pl.when(chip < last)
            def _():
                hop(a, 0, 0, split, SEAM).start()

            @pl.when(chip == last)
            def _():
                straight().start()

    @pl.when(chip == 0)
    def _():
        pl.semaphore_wait(entered.at[1], 1)
        for a, lo, size in units:
            hop(a, 0, 1, lo, size).start()

    @pl.loop(1, chips)
    def _(step):
        for a, layer in pieces:
            load(a, step, layer).start()

    @pl.loop(2, chips)
    def _(step):
        for a, layer in pieces:
            swap(a, step, layer, 1).start()

    for a in range(n):
        pltpu.make_async_copy(m_in[a], new_m[a], load_sem.at[a]).start()
        pltpu.make_async_copy(v_in[a], new_v[a], load_sem.at[a]).start()
        for layer in range(layers):
            pltpu.make_async_copy(w[a].at[layer, chip, core], old_w[a].at[layer], load_sem.at[a]).start()
    for a in range(n):
        wait_all(new_w[a].at[:, pl.ds(0, (last + 1 + 4) // CORES)], load_sem.at[a])
        wait_all(pair[a].at[1], pair_recv.at[0, a])

    @pl.loop(1, last)
    def _(step):
        @pl.when(step == 2)
        def _():
            for a in range(n):
                wait_all(pair[a].at[pl.ds(2, chips - 2)], pair_recv.at[1, a])

        @pl.when(step >= SLOTS)
        def _():
            for layer in range(layers):
                spend(layer)

        for a, layer in pieces:
            if (a, layer) == (end, 0):
                short = (step == 1) & (chip == 0)

                @pl.when(short)
                def _():
                    hop(a, 0, layer, 0, split).wait_recv()
                    add(a, step, layer, None, split, SEAM)

                @pl.when(jnp.logical_not(short))
                def _():
                    hop(a, step - 1, layer).wait_recv()
                    add(a, step, layer, step - 1, split, SEAM)

                add(a, step, layer, step - 1, 0, split)
            else:
                hop(a, step - 1, layer).wait_recv()
                add(a, step, layer, step - 1, 0, slabs[a])
            hop(a, step, layer).start()
            if a == end:
                grant(layer)

    def update(a, layer, lo, size, more=None):
        @pl.loop(lo, lo + size)
        def _(i):
            grad = total(a, last, layer, i, last - 1)
            if more is not None:
                grad = grad + more(i)
            grad = grad.astype(jnp.bfloat16).astype(jnp.float32)
            new = adamw(old_w[a][layer, i].astype(jnp.float32), new_m[a][layer, i], new_v[a][layer, i], grad)
            new_w[a][layer, chip, core, i], new_m[a][layer, i], new_v[a][layer, i] = new

    for layer in range(layers):
        spend(layer)
    for a, layer in pieces:
        hop(a, last - 1, layer).wait_recv()

        if (a, layer) == (end, 0):
            update(a, layer, 0, split)

            @pl.when(chip == last - 1)
            def _():
                straight().wait_recv()
                update(a, layer, split, SEAM, lambda i: extra[i - split].astype(jnp.float32))

            @pl.when(chip != last - 1)
            def _():
                update(a, layer, split, SEAM)

        else:
            update(a, layer, 0, slabs[a])
        spread(a, 0, layer).start()
        share(a, 0, layer).start()
        if a == end:
            grant(layer)
            if layer == 0:

                @pl.when(chip == 1)
                def _():
                    detour(0).start()

    @pl.loop(1, last - 1)
    def _(step):
        for layer in range(layers):
            spend(layer)
        for a, layer in pieces:
            spread(a, step - 1, layer).wait_recv()
            spread(a, step, layer).start()
            share(a, step, layer).start()
            if a == end:

                @pl.when(step <= last - SLOTS)
                def _():
                    grant(layer)

    for layer in range(layers):
        spend(layer)
    for a, layer in pieces:
        spread(a, last - 2, layer).wait_recv()
        if a < end:
            spread(a, last - 1, layer).start()
        else:
            if layer == 0:

                @pl.when(chip < last)
                def _():
                    spread_tail(last - 1, 0, 0).start()

            for k in range(1 - layer, len(tail[layer])):
                spread_tail(last - 1, layer, k).start()
        share(a, last - 1, layer).start()

    for a in range(end):
        for layer in range(layers):
            spread(a, last - 1, layer).wait_recv()
            share(a, last, layer).start()
    for k in range(PARTS + 1):
        for layer in range(layers):
            if k < len(tail[layer]):
                spread_tail(last, layer, k).wait_recv()
                share(end, last, layer, *tail[layer][k]).start()

    @pl.when(chip < last)
    def _():
        spread_tail(last - 1, 0, 0).wait_send()

    @pl.when(chip == 1)
    def _():
        detour(0).wait_send()

    for layer in range(layers):
        lo, size = 0, whole - (0 if layer else DETOUR)
        wait_all(new_w[end].at[layer, 0, 0, pl.ds(lo, size)], tail_send.at[layer])
    for a in range(n):
        wait_all(new_w[a], swap_send.at[a])
        wait_all(ring[a], ring_send.at[a])
        wait_all(ring[a] if a < end else ring[a].at[pl.ds(0, last - 1)], gather_send.at[a])
    for a in range(n):
        wait_all(pair[a], share_recv.at[a])


def write(n, *refs):
    *refs, sem = refs
    sources, targets = refs[: 3 * n], refs[3 * n :]
    copies = [
        pltpu.make_async_copy(source, target, sem.at[min(k, n)]) for k, (source, target) in enumerate(zip(sources, targets, strict=True))
    ]
    for copy in copies:
        copy.start()
    for copy in copies[:n]:
        copy.wait()
    part = sources[0].at[:, pl.ds(0, 2 * n)]
    pltpu.make_async_copy(part, part, sem.at[n]).wait()


def solution(mesh):
    chips = mesh.shape["dp"] // CORES

    def step(*arrays):
        terms, weights, m, v = (arrays[i : i + 3] for i in (0, 3, 6, 9))
        n, layers = len(terms), weights[0].shape[0]
        tiles = [(one.shape[1] // SUBLANES, SUBLANES, one.shape[2]) for one in m]
        whole = [(layers, chips, CORES, *tile) for tile in tiles]
        state = [(layers, *tile) for tile in tiles]
        operands = [one.reshape(shape) for one, shape in zip(terms, whole, strict=True)]
        operands += [one.reshape(shape) for one, shape in zip(weights, whole, strict=True)]
        operands += [one.reshape(shape) for part in (m, v) for one, shape in zip(part, state, strict=True)]
        sems = lambda *shape: pltpu.SemaphoreType.DMA(shape)
        vmem = lambda lead, dtype: [pltpu.VMEM((*lead, *tile), dtype) for tile in tiles]
        out = pl.pallas_call(
            functools.partial(kernel, n, chips, layers),
            out_shape=[pltpu.VMEM(shape, jnp.bfloat16) for shape in whole] + [pltpu.VMEM(shape, jnp.float32) for shape in state] * 2,
            in_specs=[pl.BlockSpec(memory_space=pl.ANY)] * len(operands),
            out_specs=[pl.BlockSpec(memory_space=pltpu.VMEM)] * (3 * n),
            scratch_shapes=[
                *vmem((chips, layers), jnp.bfloat16),
                *vmem((chips, layers), jnp.bfloat16),
                *vmem((chips - 1, layers), jnp.bfloat16),
                *vmem((layers,), jnp.bfloat16),
                *vmem((layers,), jnp.bfloat16),
                pltpu.VMEM((SEAM, *tiles[-1][1:]), jnp.bfloat16),
                sems(n + 1),
                sems(n + 1),
                sems(n),
                sems(n + 1, layers),
                sems(2, n),
                sems(n, SLOTS, layers),
                sems(PARTS + 1, layers),
                pltpu.SemaphoreType.DMA,
                sems(n),
                sems(n),
                sems(n),
                sems(n),
                sems(layers + 2),
                pltpu.SemaphoreType.REGULAR((layers,)),
                pltpu.SemaphoreType.REGULAR((3,)),
            ],
            compiler_params=pltpu.CompilerParams(collective_id=0, has_side_effects=True, vmem_limit_bytes=40 << 20),
            name="step",
        )(*operands)
        out = pl.pallas_call(
            functools.partial(write, n),
            out_shape=[jax.ShapeDtypeStruct(one.shape, one.dtype) for one in out],
            in_specs=[pl.BlockSpec(memory_space=pltpu.VMEM)] * len(out),
            out_specs=[pl.BlockSpec(memory_space=pl.ANY)] * len(out),
            scratch_shapes=[sems(n + 1)],
            compiler_params=pltpu.CompilerParams(vmem_limit_bytes=1 << 20),
            name="write",
        )(*[pltpu.with_memory_space_constraint(one, pltpu.VMEM) for one in out])
        return tuple(one.reshape(like.shape) for one, like in zip(out, (*weights, *m, *v), strict=True))

    all_of, cut = P(None, None, None), P(None, "dp", None)
    return jax.shard_map(
        step,
        mesh=mesh,
        in_specs=(P(("rep", "dp"), None, None, None),) * 3 + (all_of,) * 3 + (cut,) * 6,
        out_specs=(P("rep", None, None),) * 3 + (P("rep", "dp", None),) * 6,
        check_vma=False,
    )
```

```python
import functools

import jax
import jax.numpy as jnp
from jax import lax
from jax.experimental import pallas as pl
from jax.experimental.pallas import tpu as pltpu
from jax.sharding import PartitionSpec as P

MESH = pl.DeviceIdType.MESH
CORES = 2
SUBLANES = 8
HEAD = 1
PARTS = 4
SEAM = 10
LIFT = 9
DETOUR = 10
SLOTS = 3


def adamw(w, m, v, g):
    m = 0.9 * m + 0.1 * g
    v = 0.95 * v + 0.05 * g * g
    step = m * lax.rsqrt(v + 1e-8) + 0.1 * w
    return (w - 0.02 * step).astype(jnp.bfloat16), m, v


def cuts(count, parts):
    edges = [count * i // parts for i in range(parts + 1)]
    return [(lo, hi - lo) for lo, hi in zip(edges, edges[1:])]


def kernel(n, chips, layers, *refs):
    refs = iter(refs)
    take = lambda count: [next(refs) for _ in range(count)]
    g, w, m_in, v_in = take(n), take(n), take(n), take(n)
    new_w, new_m, new_v = take(n), take(n), take(n)
    own, pair, ring, stage, old_w, extra = take(n), take(n), take(n), take(n), take(n), take(2)
    stage_sem, first_load, load_sem, first_recv, pair_recv, ring_recv, tail_recv, extra_recv, share_recv, swap_send, ring_send, gather_send, tail_send, credit, entered = take(15)

    me = lax.axis_index("dp")
    chip, core = me // CORES, me % CORES
    other = 1 - core
    last = chips - 1
    partner = {"dp": chip * CORES + other}
    right = {"dp": (chip + 1) % chips * CORES + core}
    left = {"dp": (chip + last) % chips * CORES + core}
    ahead = [left if layer % 2 else right for layer in range(layers)]
    behind = [right if layer % 2 else left for layer in range(layers)]
    slabs = [one.shape[2] for one in own]
    end = n - 1
    whole = slabs[end]
    giver, taker = (last, 1), (last - 1, 2)
    split = [whole - SEAM, whole - LIFT]
    pieces = [(a, layer) for a in range(n) for layer in range(layers)]
    units = [(0, 0, HEAD), (0, HEAD, slabs[0] - HEAD)] + [(a, 0, slabs[a]) for a in range(1, n)]

    def block(step, layer):
        return (chip + 1 + step if layer % 2 else chip + chips - 1 - step) % chips

    def source(step, layer):
        return (chip + step if layer % 2 else chip + chips - step) % chips

    def prepare(u, layer):
        a, lo, size = units[u]
        return pltpu.make_async_copy(
            g[a].at[layer, block(0, layer), other, pl.ds(lo, size)], stage[a].at[layer, pl.ds(lo, size)], stage_sem.at[u]
        )

    def first_own(u, layer):
        a, lo, size = units[u]
        return pltpu.make_async_copy(
            g[a].at[layer, block(0, layer), core, pl.ds(lo, size)], own[a].at[0, layer, pl.ds(lo, size)], first_load.at[u]
        )

    def first_swap(u, layer):
        a, lo, size = units[u]
        return pltpu.make_async_remote_copy(
            stage[a].at[layer, pl.ds(lo, size)], pair[a].at[0, layer, pl.ds(lo, size)], swap_send.at[a], first_recv.at[u, layer], partner, MESH
        )

    def load(a, step, layer):
        return pltpu.make_async_copy(g[a].at[layer, block(step, layer), core], own[a].at[step, layer], load_sem.at[a])

    def swap(a, step, layer, sem):
        return pltpu.make_async_remote_copy(
            g[a].at[layer, block(step, layer), other], pair[a].at[step, layer], swap_send.at[a], pair_recv.at[sem, a], partner, MESH
        )

    def hop(a, step, layer, lo=0, size=None):
        part = pl.ds(lo, slabs[a] if size is None else size)
        return pltpu.make_async_remote_copy(
            own[a].at[step, layer, part],
            ring[a].at[step, layer, part],
            ring_send.at[a],
            ring_recv.at[a, step % SLOTS, layer],
            ahead[layer],
            MESH,
        )

    def spread(a, step, layer):
        here = new_w[a].at[layer, source(step, layer), core]
        return pltpu.make_async_remote_copy(
            here, here, gather_send.at[a], ring_recv.at[a, (step + last) % SLOTS, layer], ahead[layer], MESH
        )

    def straight(layer):
        part = pl.ds(split[layer], whole - split[layer])
        return pltpu.make_async_remote_copy(
            own[end].at[0, layer, part], extra[layer], ring_send.at[end], extra_recv.at[layer], behind[layer], MESH
        )

    tail = [cuts(whole, PARTS) if layer else [(whole - DETOUR, DETOUR), *cuts(whole - DETOUR, PARTS)] for layer in range(layers)]

    def spread_tail(step, layer, k):
        here = new_w[end].at[layer, source(step, layer), core, pl.ds(*tail[layer][k])]
        sem = tail_send.at[layers if layer == k == 0 else layer]
        return pltpu.make_async_remote_copy(here, here, sem, tail_recv.at[k, layer], ahead[layer], MESH)

    def detour(step):
        here = new_w[end].at[0, source(step, 0), core, pl.ds(*tail[0][0])]
        return pltpu.make_async_remote_copy(here, here, tail_send.at[layers + 1], tail_recv.at[0, 0], left, MESH)

    def share(a, step, layer, lo=0, size=None):
        here = new_w[a].at[layer, source(step, layer), core, pl.ds(lo, slabs[a] if size is None else size)]
        return pltpu.make_async_remote_copy(here, here, swap_send.at[a], share_recv.at[a], partner, MESH)

    def wait_all(here, sem):
        pltpu.make_async_copy(here, here, sem).wait()

    def grant(layer):
        pl.semaphore_signal(credit.at[layer], inc=1, device_id=behind[layer], device_id_type=MESH)

    def spend(layer):
        pl.semaphore_wait(credit.at[layer], 1)

    for layer in range(layers):
        prepare(0, layer).start()
    for layer in range(layers):
        first_own(0, layer).start()
    barrier = pltpu.get_barrier_semaphore()

    def greet(device):
        pl.semaphore_signal(barrier, inc=1, device_id=device, device_id_type=MESH)

    def answer(which, device):
        pl.semaphore_signal(entered.at[which], inc=1, device_id=device, device_id_type=MESH)

    def answer_chips():
        @pl.when(chip > 0)
        def _():
            answer(0, left)

        @pl.when(chip == last)
        def _():
            answer(1, right)

    greeted = jnp.where(chip > 0, 1, 0) + jnp.where(chip == last, 1, 0)
    pl.when(chip < last)(lambda: greet(right))
    pl.when(chip == 0)(lambda: greet(left))
    pl.when(core == 0)(lambda: greet(partner))
    for u in range(1, n + 1):
        for layer in range(layers):
            prepare(u, layer).start()

    @pl.when(core > 0)
    def _():
        pl.semaphore_wait(barrier, greeted + 1)
        answer(2, partner)
        answer_chips()

    @pl.when(core == 0)
    def _():
        pl.semaphore_wait(entered.at[2], 1)

    for u, (a, lo, size) in enumerate(units):
        wait_all(stage[a].at[:, pl.ds(lo, size)], stage_sem.at[u])
        for layer in range(layers):
            first_swap(u, layer).start()
        if u:
            for layer in range(layers):
                first_own(u, layer).start()
    for a, layer in pieces:
        swap(a, 1, layer, 0).start()

    @pl.when(core == 0)
    def _():
        @pl.when(chip > 0)
        def _():
            pl.semaphore_wait(barrier, greeted)

        answer_chips()

    def total(a, step, layer, i, arrived):
        t = own[a][step, layer, i].astype(jnp.float32) + pair[a][step, layer, i].astype(jnp.float32)
        if arrived is not None:
            t = t + ring[a][arrived, layer, i].astype(jnp.float32)
        return t

    def add(a, step, layer, arrived, lo, size):
        @pl.loop(lo, lo + size)
        def _(i):
            own[a][step, layer, i] = total(a, step, layer, i, arrived).astype(jnp.bfloat16)

    for u, (a, lo, size) in enumerate(units):
        wait_all(own[a].at[0, :, pl.ds(lo, size)], first_load.at[u])
        for layer in range(layers):
            first_swap(u, layer).wait_recv()
            add(a, 0, layer, None, lo, size)

        def send(layer):
            if a < end:
                hop(a, 0, layer, lo, size).start()
                return
            hop(a, 0, layer, 0, split[layer]).start()

            @pl.when(chip != giver[layer])
            def _():
                hop(a, 0, layer, split[layer], whole - split[layer]).start()

            @pl.when(chip == giver[layer])
            def _():
                straight(layer).start()

        @pl.when(chip > 0)
        def _():
            send(1)

        if u == 0:

            @pl.when(chip < last)
            def _():
                pl.semaphore_wait(entered.at[0], 1)

        send(0)

    @pl.when(chip == 0)
    def _():
        pl.semaphore_wait(entered.at[1], 1)
        for a, lo, size in units:
            hop(a, 0, 1, lo, size).start()

    @pl.loop(1, chips)
    def _(step):
        for a, layer in pieces:
            load(a, step, layer).start()

    @pl.loop(2, chips)
    def _(step):
        for a, layer in pieces:
            swap(a, step, layer, 1).start()

    for a in range(n):
        pltpu.make_async_copy(m_in[a], new_m[a], load_sem.at[a]).start()
        pltpu.make_async_copy(v_in[a], new_v[a], load_sem.at[a]).start()
        for layer in range(layers):
            pltpu.make_async_copy(w[a].at[layer, chip, core], old_w[a].at[layer], load_sem.at[a]).start()
    for a in range(n):
        wait_all(new_w[a].at[:, pl.ds(0, (last + 1 + 4) // CORES)], load_sem.at[a])
        wait_all(pair[a].at[1], pair_recv.at[0, a])

    @pl.loop(1, last)
    def _(step):
        @pl.when(step == 2)
        def _():
            for a in range(n):
                wait_all(pair[a].at[pl.ds(2, chips - 2)], pair_recv.at[1, a])

        @pl.when(step >= SLOTS)
        def _():
            for layer in range(layers):
                spend(layer)

        for a, layer in pieces:
            if a == end:
                short = (step == 1) & (chip == 0)
                cut = split[layer]

                @pl.when(short)
                def _():
                    hop(a, 0, layer, 0, cut).wait_recv()
                    add(a, step, layer, None, cut, whole - cut)

                @pl.when(jnp.logical_not(short))
                def _():
                    hop(a, step - 1, layer).wait_recv()
                    add(a, step, layer, step - 1, cut, whole - cut)

                add(a, step, layer, step - 1, 0, cut)
            else:
                hop(a, step - 1, layer).wait_recv()
                add(a, step, layer, step - 1, 0, slabs[a])
            hop(a, step, layer).start()
            if a == end:
                grant(layer)

    def update(a, layer, lo, size, more=None):
        @pl.loop(lo, lo + size)
        def _(i):
            grad = total(a, last, layer, i, last - 1)
            if more is not None:
                grad = grad + more(i)
            grad = grad.astype(jnp.bfloat16).astype(jnp.float32)
            new = adamw(old_w[a][layer, i].astype(jnp.float32), new_m[a][layer, i], new_v[a][layer, i], grad)
            new_w[a][layer, chip, core, i], new_m[a][layer, i], new_v[a][layer, i] = new

    for layer in range(layers):
        spend(layer)
    for a, layer in pieces:
        hop(a, last - 1, layer).wait_recv()

        if a == end:
            cut = split[layer]
            update(a, layer, 0, cut)

            @pl.when(chip == taker[layer])
            def _():
                straight(layer).wait_recv()
                update(a, layer, cut, whole - cut, lambda i: extra[layer][i - cut].astype(jnp.float32))

            @pl.when(chip != taker[layer])
            def _():
                update(a, layer, cut, whole - cut)

        else:
            update(a, layer, 0, slabs[a])
        spread(a, 0, layer).start()
        share(a, 0, layer).start()
        if a == end:
            grant(layer)
            if layer == 0:

                @pl.when(chip == 1)
                def _():
                    detour(0).start()

    @pl.loop(1, last - 1)
    def _(step):
        for layer in range(layers):
            spend(layer)
        for a, layer in pieces:
            spread(a, step - 1, layer).wait_recv()
            spread(a, step, layer).start()
            share(a, step, layer).start()
            if a == end:

                @pl.when(step <= last - SLOTS)
                def _():
                    grant(layer)

    for layer in range(layers):
        spend(layer)
    for a, layer in pieces:
        spread(a, last - 2, layer).wait_recv()
        if a < end:
            spread(a, last - 1, layer).start()
        else:
            if layer == 0:

                @pl.when(chip < last)
                def _():
                    spread_tail(last - 1, 0, 0).start()

            for k in range(1 - layer, len(tail[layer])):
                spread_tail(last - 1, layer, k).start()
        share(a, last - 1, layer).start()

    for a in range(end):
        for layer in range(layers):
            spread(a, last - 1, layer).wait_recv()
            share(a, last, layer).start()
    for k in range(PARTS + 1):
        for layer in range(layers):
            if k < len(tail[layer]):
                spread_tail(last, layer, k).wait_recv()
                share(end, last, layer, *tail[layer][k]).start()

    @pl.when(chip < last)
    def _():
        spread_tail(last - 1, 0, 0).wait_send()

    @pl.when(chip == 1)
    def _():
        detour(0).wait_send()

    for layer in range(layers):
        lo, size = 0, whole - (0 if layer else DETOUR)
        wait_all(new_w[end].at[layer, 0, 0, pl.ds(lo, size)], tail_send.at[layer])
    for a in range(n):
        wait_all(new_w[a], swap_send.at[a])
        wait_all(ring[a], ring_send.at[a])
        wait_all(ring[a] if a < end else ring[a].at[pl.ds(0, last - 1)], gather_send.at[a])
    for a in range(n):
        wait_all(pair[a], share_recv.at[a])


def write(n, *refs):
    *refs, sem = refs
    sources, targets = refs[: 3 * n], refs[3 * n :]
    copies = [
        pltpu.make_async_copy(source, target, sem.at[min(k, n)]) for k, (source, target) in enumerate(zip(sources, targets, strict=True))
    ]
    for copy in copies:
        copy.start()
    for copy in copies[:n]:
        copy.wait()
    part = sources[0].at[:, pl.ds(0, 2 * n)]
    pltpu.make_async_copy(part, part, sem.at[n]).wait()


def solution(mesh):
    chips = mesh.shape["dp"] // CORES

    def step(*arrays):
        terms, weights, m, v = (arrays[i : i + 3] for i in (0, 3, 6, 9))
        n, layers = len(terms), weights[0].shape[0]
        tiles = [(one.shape[1] // SUBLANES, SUBLANES, one.shape[2]) for one in m]
        whole = [(layers, chips, CORES, *tile) for tile in tiles]
        state = [(layers, *tile) for tile in tiles]
        operands = [one.reshape(shape) for one, shape in zip(terms, whole, strict=True)]
        operands += [one.reshape(shape) for one, shape in zip(weights, whole, strict=True)]
        operands += [one.reshape(shape) for part in (m, v) for one, shape in zip(part, state, strict=True)]
        sems = lambda *shape: pltpu.SemaphoreType.DMA(shape)
        vmem = lambda lead, dtype: [pltpu.VMEM((*lead, *tile), dtype) for tile in tiles]
        out = pl.pallas_call(
            functools.partial(kernel, n, chips, layers),
            out_shape=[pltpu.VMEM(shape, jnp.bfloat16) for shape in whole] + [pltpu.VMEM(shape, jnp.float32) for shape in state] * 2,
            in_specs=[pl.BlockSpec(memory_space=pl.ANY)] * len(operands),
            out_specs=[pl.BlockSpec(memory_space=pltpu.VMEM)] * (3 * n),
            scratch_shapes=[
                *vmem((chips, layers), jnp.bfloat16),
                *vmem((chips, layers), jnp.bfloat16),
                *vmem((chips - 1, layers), jnp.bfloat16),
                *vmem((layers,), jnp.bfloat16),
                *vmem((layers,), jnp.bfloat16),
                *[pltpu.VMEM((slabs, *tiles[-1][1:]), jnp.bfloat16) for slabs in (SEAM, LIFT)],
                sems(n + 1),
                sems(n + 1),
                sems(n),
                sems(n + 1, layers),
                sems(2, n),
                sems(n, SLOTS, layers),
                sems(PARTS + 1, layers),
                sems(layers),
                sems(n),
                sems(n),
                sems(n),
                sems(n),
                sems(layers + 2),
                pltpu.SemaphoreType.REGULAR((layers,)),
                pltpu.SemaphoreType.REGULAR((3,)),
            ],
            compiler_params=pltpu.CompilerParams(collective_id=0, has_side_effects=True, vmem_limit_bytes=40 << 20),
            name="step",
        )(*operands)
        out = pl.pallas_call(
            functools.partial(write, n),
            out_shape=[jax.ShapeDtypeStruct(one.shape, one.dtype) for one in out],
            in_specs=[pl.BlockSpec(memory_space=pltpu.VMEM)] * len(out),
            out_specs=[pl.BlockSpec(memory_space=pl.ANY)] * len(out),
            scratch_shapes=[sems(n + 1)],
            compiler_params=pltpu.CompilerParams(vmem_limit_bytes=1 << 20),
            name="write",
        )(*[pltpu.with_memory_space_constraint(one, pltpu.VMEM) for one in out])
        return tuple(one.reshape(like.shape) for one, like in zip(out, (*weights, *m, *v), strict=True))

    all_of, cut = P(None, None, None), P(None, "dp", None)
    return jax.shard_map(
        step,
        mesh=mesh,
        in_specs=(P(("rep", "dp"), None, None, None),) * 3 + (all_of,) * 3 + (cut,) * 6,
        out_specs=(P("rep", None, None),) * 3 + (P("rep", "dp", None),) * 6,
        check_vma=False,
    )
```

```python
import functools

import jax
import jax.numpy as jnp
from jax import lax
from jax.experimental import pallas as pl
from jax.experimental.pallas import tpu as pltpu
from jax.sharding import PartitionSpec as P

MESH = pl.DeviceIdType.MESH
CORES = 2
SUBLANES = 8
HEAD = 1
PARTS = 2
SEAM = 10
LIFT = 9
DETOUR = 10
SLOTS = 3


def adamw(w, m, v, g):
    m = 0.9 * m + 0.1 * g
    v = 0.95 * v + 0.05 * g * g
    step = m * lax.rsqrt(v + 1e-8) + 0.1 * w
    return (w - 0.02 * step).astype(jnp.bfloat16), m, v


def cuts(count, parts):
    edges = [count * i // parts for i in range(parts + 1)]
    return [(lo, hi - lo) for lo, hi in zip(edges, edges[1:])]


def kernel(n, chips, layers, *refs):
    refs = iter(refs)
    take = lambda count: [next(refs) for _ in range(count)]
    g, w, m_in, v_in = take(n), take(n), take(n), take(n)
    new_w, new_m, new_v = take(n), take(n), take(n)
    own, pair, ring, stage, old_w, extra = take(n), take(n), take(n), take(n), take(n), take(2)
    stage_sem, first_load, load_sem, first_recv, pair_recv, ring_recv, tail_recv, extra_recv, share_recv, swap_send, ring_send, gather_send, tail_send, credit, entered = take(15)

    me = lax.axis_index("dp")
    chip, core = me // CORES, me % CORES
    other = 1 - core
    last = chips - 1
    partner = {"dp": chip * CORES + other}
    right = {"dp": (chip + 1) % chips * CORES + core}
    left = {"dp": (chip + last) % chips * CORES + core}
    ahead = [left if layer % 2 else right for layer in range(layers)]
    behind = [right if layer % 2 else left for layer in range(layers)]
    slabs = [one.shape[2] for one in own]
    end = n - 1
    whole = slabs[end]
    giver, taker = (last, 1), (last - 1, 2)
    split = [whole - SEAM, whole - LIFT]
    pieces = [(a, layer) for a in range(n) for layer in range(layers)]
    units = [(0, 0, HEAD), (0, HEAD, slabs[0] - HEAD)] + [(a, 0, slabs[a]) for a in range(1, n)]

    def block(step, layer):
        return (chip + 1 + step if layer % 2 else chip + chips - 1 - step) % chips

    def source(step, layer):
        return (chip + step if layer % 2 else chip + chips - step) % chips

    def prepare(u, layer):
        a, lo, size = units[u]
        return pltpu.make_async_copy(
            g[a].at[layer, block(0, layer), other, pl.ds(lo, size)], stage[a].at[layer, pl.ds(lo, size)], stage_sem.at[u]
        )

    def first_own(u, layer):
        a, lo, size = units[u]
        return pltpu.make_async_copy(
            g[a].at[layer, block(0, layer), core, pl.ds(lo, size)], own[a].at[0, layer, pl.ds(lo, size)], first_load.at[u]
        )

    def first_swap(u, layer):
        a, lo, size = units[u]
        return pltpu.make_async_remote_copy(
            stage[a].at[layer, pl.ds(lo, size)], pair[a].at[0, layer, pl.ds(lo, size)], swap_send.at[a], first_recv.at[u], partner, MESH
        )

    def load(a, step, layer):
        return pltpu.make_async_copy(g[a].at[layer, block(step, layer), core], own[a].at[step, layer], load_sem.at[a])

    def swap(a, step, layer, sem):
        return pltpu.make_async_remote_copy(
            g[a].at[layer, block(step, layer), other], pair[a].at[step, layer], swap_send.at[a], pair_recv.at[sem, a], partner, MESH
        )

    def hop(a, step, layer, lo=0, size=None):
        part = pl.ds(lo, slabs[a] if size is None else size)
        return pltpu.make_async_remote_copy(
            own[a].at[step, layer, part],
            ring[a].at[step, layer, part],
            ring_send.at[a],
            ring_recv.at[a, step % SLOTS, layer],
            ahead[layer],
            MESH,
        )

    def spread(a, step, layer):
        here = new_w[a].at[layer, source(step, layer), core]
        return pltpu.make_async_remote_copy(
            here, here, ring_send.at[a] if a < end else gather_send, ring_recv.at[a, (step + last) % SLOTS, layer], ahead[layer], MESH
        )

    def straight(layer):
        part = pl.ds(split[layer], whole - split[layer])
        return pltpu.make_async_remote_copy(
            own[end].at[0, layer, part], extra[layer], ring_send.at[end], extra_recv.at[layer], behind[layer], MESH
        )

    tail = [cuts(whole, PARTS) if layer else [(whole - DETOUR, DETOUR), *cuts(whole - DETOUR, PARTS)] for layer in range(layers)]

    def spread_tail(step, layer, k):
        here = new_w[end].at[layer, source(step, layer), core, pl.ds(*tail[layer][k])]
        sem = tail_send.at[layers if layer == k == 0 else layer]
        return pltpu.make_async_remote_copy(here, here, sem, tail_recv.at[k, layer], ahead[layer], MESH)

    def detour(step):
        here = new_w[end].at[0, source(step, 0), core, pl.ds(*tail[0][0])]
        return pltpu.make_async_remote_copy(here, here, tail_send.at[layers + 1], tail_recv.at[0, 0], left, MESH)

    def share(a, step, layer, lo=0, size=None):
        here = new_w[a].at[layer, source(step, layer), core, pl.ds(lo, slabs[a] if size is None else size)]
        return pltpu.make_async_remote_copy(here, here, swap_send.at[a], share_recv.at[a], partner, MESH)

    def wait_all(here, sem):
        pltpu.make_async_copy(here, here, sem).wait()

    def grant(layer):
        pl.semaphore_signal(credit.at[layer], inc=1, device_id=behind[layer], device_id_type=MESH)

    def spend(layer):
        pl.semaphore_wait(credit.at[layer], 1)

    for layer in range(layers):
        prepare(0, layer).start()
    for layer in range(layers):
        first_own(0, layer).start()
    barrier = pltpu.get_barrier_semaphore()

    def greet(device):
        pl.semaphore_signal(barrier, inc=1, device_id=device, device_id_type=MESH)

    def answer(which, device):
        pl.semaphore_signal(entered.at[which], inc=1, device_id=device, device_id_type=MESH)

    def answer_chips():
        @pl.when(chip > 0)
        def _():
            answer(0, left)

        @pl.when(chip == last)
        def _():
            answer(1, right)

    greeted = jnp.where(chip > 0, 1, 0) + jnp.where(chip == last, 1, 0)
    pl.when(chip < last)(lambda: greet(right))
    pl.when(chip == 0)(lambda: greet(left))
    pl.when(core == 0)(lambda: greet(partner))
    for u in range(1, n + 1):
        for layer in range(layers):
            prepare(u, layer).start()

    @pl.when(core > 0)
    def _():
        pl.semaphore_wait(barrier, greeted + 1)
        answer(2, partner)
        answer_chips()

    @pl.when(core == 0)
    def _():
        pl.semaphore_wait(entered.at[2], 1)

    for u, (a, lo, size) in enumerate(units):
        wait_all(stage[a].at[:, pl.ds(lo, size)], stage_sem.at[u])
        for layer in range(layers):
            first_swap(u, layer).start()
        if u:
            for layer in range(layers):
                first_own(u, layer).start()
    for a, layer in pieces:
        swap(a, 1, layer, 0).start()

    @pl.when(core == 0)
    def _():
        @pl.when(chip > 0)
        def _():
            pl.semaphore_wait(barrier, greeted)

        answer_chips()

    def total(a, step, layer, i, arrived):
        t = own[a][step, layer, i].astype(jnp.float32) + pair[a][step, layer, i].astype(jnp.float32)
        if arrived is not None:
            t = t + ring[a][arrived, layer, i].astype(jnp.float32)
        return t

    def add(a, step, layer, arrived, lo, size):
        @pl.loop(lo, lo + size)
        def _(i):
            own[a][step, layer, i] = total(a, step, layer, i, arrived).astype(jnp.bfloat16)

    for u, (a, lo, size) in enumerate(units):
        wait_all(own[a].at[0, :, pl.ds(lo, size)], first_load.at[u])
        wait_all(pair[a].at[0, :, pl.ds(lo, size)], first_recv.at[u])
        for layer in range(layers):
            add(a, 0, layer, None, lo, size)

        def send(layer):
            if a < end:
                hop(a, 0, layer, lo, size).start()
                return
            hop(a, 0, layer, 0, split[layer]).start()

            @pl.when(chip != giver[layer])
            def _():
                hop(a, 0, layer, split[layer], whole - split[layer]).start()

            @pl.when(chip == giver[layer])
            def _():
                straight(layer).start()

        @pl.when(chip > 0)
        def _():
            send(1)

        if u == 0:

            @pl.when(chip < last)
            def _():
                pl.semaphore_wait(entered.at[0], 1)

        send(0)

    @pl.when(chip == 0)
    def _():
        pl.semaphore_wait(entered.at[1], 1)
        for a, lo, size in units:
            hop(a, 0, 1, lo, size).start()

    @pl.loop(1, chips)
    def _(step):
        for a, layer in pieces:
            load(a, step, layer).start()

    @pl.loop(2, chips)
    def _(step):
        for a, layer in pieces:
            swap(a, step, layer, 1).start()

    for a in range(n):
        pltpu.make_async_copy(m_in[a], new_m[a], load_sem.at[a]).start()
        pltpu.make_async_copy(v_in[a], new_v[a], load_sem.at[a]).start()
        for layer in range(layers):
            pltpu.make_async_copy(w[a].at[layer, chip, core], old_w[a].at[layer], load_sem.at[a]).start()
    for a in range(n):
        wait_all(new_w[a].at[:, pl.ds(0, (last + 1 + 4) // CORES)], load_sem.at[a])
        wait_all(pair[a].at[1], pair_recv.at[0, a])

    @pl.loop(1, last)
    def _(step):
        @pl.when(step == 2)
        def _():
            for a in range(n):
                wait_all(pair[a].at[pl.ds(2, chips - 2)], pair_recv.at[1, a])

        @pl.when(step >= SLOTS)
        def _():
            for layer in range(layers):
                spend(layer)

        for a, layer in pieces:
            if a == end:
                short = (step == 1) & (chip == 0)
                cut = split[layer]

                @pl.when(short)
                def _():
                    hop(a, 0, layer, 0, cut).wait_recv()
                    add(a, step, layer, None, cut, whole - cut)

                @pl.when(jnp.logical_not(short))
                def _():
                    hop(a, step - 1, layer).wait_recv()
                    add(a, step, layer, step - 1, cut, whole - cut)

                add(a, step, layer, step - 1, 0, cut)
            else:
                hop(a, step - 1, layer).wait_recv()
                add(a, step, layer, step - 1, 0, slabs[a])
            hop(a, step, layer).start()
            if a == end:
                grant(layer)

    def update(a, layer, lo, size, more=None):
        @pl.loop(lo, lo + size)
        def _(i):
            grad = total(a, last, layer, i, last - 1)
            if more is not None:
                grad = grad + more(i)
            grad = grad.astype(jnp.bfloat16).astype(jnp.float32)
            new = adamw(old_w[a][layer, i].astype(jnp.float32), new_m[a][layer, i], new_v[a][layer, i], grad)
            new_w[a][layer, chip, core, i], new_m[a][layer, i], new_v[a][layer, i] = new

    for layer in range(layers):
        spend(layer)
    for a, layer in pieces:
        hop(a, last - 1, layer).wait_recv()

        if a == end:
            cut = split[layer]
            update(a, layer, 0, cut)

            @pl.when(chip == taker[layer])
            def _():
                straight(layer).wait_recv()
                update(a, layer, cut, whole - cut, lambda i: extra[layer][i - cut].astype(jnp.float32))

            @pl.when(chip != taker[layer])
            def _():
                update(a, layer, cut, whole - cut)

        else:
            update(a, layer, 0, slabs[a])
        spread(a, 0, layer).start()
        share(a, 0, layer).start()
        if a == end:
            grant(layer)
            if layer == 0:

                @pl.when(chip == 1)
                def _():
                    detour(0).start()

    @pl.loop(1, last - 1)
    def _(step):
        for layer in range(layers):
            spend(layer)
        for a, layer in pieces:
            spread(a, step - 1, layer).wait_recv()
            spread(a, step, layer).start()
            share(a, step, layer).start()
            if a == end:

                @pl.when(step <= last - SLOTS)
                def _():
                    grant(layer)

    for layer in range(layers):
        spend(layer)
    for a, layer in pieces:
        spread(a, last - 2, layer).wait_recv()
        if a < end:
            spread(a, last - 1, layer).start()
        else:
            if layer == 0:

                @pl.when(chip < last)
                def _():
                    spread_tail(last - 1, 0, 0).start()

            for k in range(1 - layer, len(tail[layer])):
                spread_tail(last - 1, layer, k).start()
        share(a, last - 1, layer).start()

    for a in range(end):
        for layer in range(layers):
            spread(a, last - 1, layer).wait_recv()
            share(a, last, layer).start()
    for k in range(PARTS + 1):
        for layer in range(layers):
            if k < len(tail[layer]):
                spread_tail(last, layer, k).wait_recv()
                share(end, last, layer, *tail[layer][k]).start()

    @pl.when(chip < last)
    def _():
        spread_tail(last - 1, 0, 0).wait_send()

    @pl.when(chip == 1)
    def _():
        detour(0).wait_send()

    for layer in range(layers):
        lo, size = 0, whole - (0 if layer else DETOUR)
        wait_all(new_w[end].at[layer, 0, 0, pl.ds(lo, size)], tail_send.at[layer])
    for a in range(n):
        wait_all(new_w[a], swap_send.at[a])
        wait_all(new_w[a].at[:, pl.ds(0, last)] if a < end else ring[a], ring_send.at[a])
    wait_all(ring[end].at[pl.ds(0, last - 1)], gather_send)
    for a in range(n):
        wait_all(pair[a], share_recv.at[a])


def write(n, *refs):
    *refs, sem = refs
    sources, targets = refs[: 3 * n], refs[3 * n :]
    weights = list(zip(sources, targets, strict=True))[:n]
    for a, (source, target) in enumerate(weights):
        for layer in range(source.shape[0]):
            for chip in range(source.shape[1]):
                pltpu.make_async_copy(source.at[layer, chip], target.at[layer, chip], sem.at[a]).start()
    for source, target in zip(sources[n:], targets[n:], strict=True):
        pltpu.make_async_copy(source, target, sem.at[n]).start()
    for a, (source, target) in enumerate(weights):
        pltpu.make_async_copy(source, target, sem.at[a]).wait()
    part = sources[0].at[:, pl.ds(0, 2 * n)]
    pltpu.make_async_copy(part, part, sem.at[n]).wait()


def solution(mesh):
    chips = mesh.shape["dp"] // CORES

    def step(*arrays):
        terms, weights, m, v = (arrays[i : i + 3] for i in (0, 3, 6, 9))
        n, layers = len(terms), weights[0].shape[0]
        tiles = [(one.shape[1] // SUBLANES, SUBLANES, one.shape[2]) for one in m]
        whole = [(layers, chips, CORES, *tile) for tile in tiles]
        state = [(layers, *tile) for tile in tiles]
        operands = [one.reshape(shape) for one, shape in zip(terms, whole, strict=True)]
        operands += [one.reshape(shape) for one, shape in zip(weights, whole, strict=True)]
        operands += [one.reshape(shape) for part in (m, v) for one, shape in zip(part, state, strict=True)]
        sems = lambda *shape: pltpu.SemaphoreType.DMA(shape)
        vmem = lambda lead, dtype: [pltpu.VMEM((*lead, *tile), dtype) for tile in tiles]
        out = pl.pallas_call(
            functools.partial(kernel, n, chips, layers),
            out_shape=[pltpu.VMEM(shape, jnp.bfloat16) for shape in whole] + [pltpu.VMEM(shape, jnp.float32) for shape in state] * 2,
            in_specs=[pl.BlockSpec(memory_space=pl.ANY)] * len(operands),
            out_specs=[pl.BlockSpec(memory_space=pltpu.VMEM)] * (3 * n),
            scratch_shapes=[
                *vmem((chips, layers), jnp.bfloat16),
                *vmem((chips, layers), jnp.bfloat16),
                *vmem((chips - 1, layers), jnp.bfloat16),
                *vmem((layers,), jnp.bfloat16),
                *vmem((layers,), jnp.bfloat16),
                *[pltpu.VMEM((slabs, *tiles[-1][1:]), jnp.bfloat16) for slabs in (SEAM, LIFT)],
                sems(n + 1),
                sems(n + 1),
                sems(n),
                sems(n + 1),
                sems(2, n),
                sems(n, SLOTS, layers),
                sems(PARTS + 1, layers),
                sems(layers),
                sems(n),
                sems(n),
                sems(n),
                pltpu.SemaphoreType.DMA,
                sems(layers + 2),
                pltpu.SemaphoreType.REGULAR((layers,)),
                pltpu.SemaphoreType.REGULAR((3,)),
            ],
            compiler_params=pltpu.CompilerParams(collective_id=0, has_side_effects=True, vmem_limit_bytes=40 << 20),
            name="step",
        )(*operands)
        out = pl.pallas_call(
            functools.partial(write, n),
            out_shape=[jax.ShapeDtypeStruct(one.shape, one.dtype) for one in out],
            in_specs=[pl.BlockSpec(memory_space=pltpu.VMEM)] * len(out),
            out_specs=[pl.BlockSpec(memory_space=pl.ANY)] * len(out),
            scratch_shapes=[sems(n + 1)],
            compiler_params=pltpu.CompilerParams(vmem_limit_bytes=1 << 20),
            name="write",
        )(*[pltpu.with_memory_space_constraint(one, pltpu.VMEM) for one in out])
        return tuple(one.reshape(like.shape) for one, like in zip(out, (*weights, *m, *v), strict=True))

    all_of, cut = P(None, None, None), P(None, "dp", None)
    return jax.shard_map(
        step,
        mesh=mesh,
        in_specs=(P(("rep", "dp"), None, None, None),) * 3 + (all_of,) * 3 + (cut,) * 6,
        out_specs=(P("rep", None, None),) * 3 + (P("rep", "dp", None),) * 6,
        check_vma=False,
    )
```

```python
import functools

import jax
import jax.numpy as jnp
from jax import lax
from jax.experimental import pallas as pl
from jax.experimental.pallas import tpu as pltpu
from jax.sharding import PartitionSpec as P

MESH = pl.DeviceIdType.MESH
CORES = 2
SUBLANES = 8
HEAD = 1
PARTS = 2
SEAM = 10
LIFT = 12
DETOUR = (12, 4)
SLOTS = 3


def adamw(w, m, v, g):
    m = 0.9 * m + 0.1 * g
    v = 0.95 * v + 0.05 * g * g
    step = m * lax.rsqrt(v + 1e-8) + 0.1 * w
    return (w - 0.02 * step).astype(jnp.bfloat16), m, v


def cuts(count, parts):
    edges = [count * i // parts for i in range(parts + 1)]
    return [(lo, hi - lo) for lo, hi in zip(edges, edges[1:])]


def kernel(n, chips, layers, *refs):
    refs = iter(refs)
    take = lambda count: [next(refs) for _ in range(count)]
    g, w, m_in, v_in = take(n), take(n), take(n), take(n)
    new_w, new_m, new_v = take(n), take(n), take(n)
    own, pair, ring, stage, old_w, extra = take(n), take(n), take(n), take(n), take(n), take(2)
    stage_sem, first_load, load_sem, first_recv, pair_recv, ring_recv, tail_recv, extra_recv, share_recv, swap_send, ring_send, gather_send, tail_send, credit, entered = take(15)

    me = lax.axis_index("dp")
    chip, core = me // CORES, me % CORES
    other = 1 - core
    last = chips - 1
    partner = {"dp": chip * CORES + other}
    right = {"dp": (chip + 1) % chips * CORES + core}
    left = {"dp": (chip + last) % chips * CORES + core}
    ahead = [left if layer % 2 else right for layer in range(layers)]
    behind = [right if layer % 2 else left for layer in range(layers)]
    slabs = [one.shape[2] for one in own]
    end = n - 1
    whole = slabs[end]
    giver, taker = (last, 1), (last - 1, 2)
    split = [whole - SEAM, whole - LIFT]
    pieces = [(a, layer) for a in range(n) for layer in range(layers)]
    units = [(0, 0, HEAD), (0, HEAD, slabs[0] - HEAD)] + [(a, 0, slabs[a]) for a in range(1, n)]

    def block(step, layer):
        return (chip + 1 + step if layer % 2 else chip + chips - 1 - step) % chips

    def source(step, layer):
        return (chip + step if layer % 2 else chip + chips - step) % chips

    def prepare(u, layer):
        a, lo, size = units[u]
        return pltpu.make_async_copy(
            g[a].at[layer, block(0, layer), other, pl.ds(lo, size)], stage[a].at[layer, pl.ds(lo, size)], stage_sem.at[u]
        )

    def first_own(u, layer):
        a, lo, size = units[u]
        return pltpu.make_async_copy(
            g[a].at[layer, block(0, layer), core, pl.ds(lo, size)], own[a].at[0, layer, pl.ds(lo, size)], first_load.at[u]
        )

    def first_swap(u, layer):
        a, lo, size = units[u]
        return pltpu.make_async_remote_copy(
            stage[a].at[layer, pl.ds(lo, size)], pair[a].at[0, layer, pl.ds(lo, size)], swap_send.at[a], first_recv.at[u], partner, MESH
        )

    def load(a, step, layer):
        return pltpu.make_async_copy(g[a].at[layer, block(step, layer), core], own[a].at[step, layer], load_sem.at[a])

    def swap(a, step, layer, sem):
        return pltpu.make_async_remote_copy(
            g[a].at[layer, block(step, layer), other], pair[a].at[step, layer], swap_send.at[a], pair_recv.at[sem, a], partner, MESH
        )

    def hop(a, step, layer, lo=0, size=None):
        part = pl.ds(lo, slabs[a] if size is None else size)
        return pltpu.make_async_remote_copy(
            own[a].at[step, layer, part],
            ring[a].at[step, layer, part],
            ring_send.at[a],
            ring_recv.at[a, step % SLOTS, layer],
            ahead[layer],
            MESH,
        )

    def spread(a, step, layer):
        here = new_w[a].at[layer, source(step, layer), core]
        return pltpu.make_async_remote_copy(
            here, here, ring_send.at[a] if a < end else gather_send, ring_recv.at[a, (step + last) % SLOTS, layer], ahead[layer], MESH
        )

    def straight(layer):
        part = pl.ds(split[layer], whole - split[layer])
        return pltpu.make_async_remote_copy(
            own[end].at[0, layer, part], extra[layer], ring_send.at[end], extra_recv.at[layer], behind[layer], MESH
        )

    sender, keeper = (1, last - 1), (last, 0)
    tail = [[(whole - skip, skip), *cuts(whole - skip, PARTS)] for skip in DETOUR]

    def spread_tail(step, layer, k):
        here = new_w[end].at[layer, source(step, layer), core, pl.ds(*tail[layer][k])]
        sem = tail_send.at[0 if k else 1, layer]
        return pltpu.make_async_remote_copy(here, here, sem, tail_recv.at[k, layer], ahead[layer], MESH)

    def detour(layer):
        here = new_w[end].at[layer, chip, core, pl.ds(*tail[layer][0])]
        return pltpu.make_async_remote_copy(here, here, tail_send.at[2, layer], tail_recv.at[0, layer], behind[layer], MESH)

    def share(a, step, layer, lo=0, size=None):
        here = new_w[a].at[layer, source(step, layer), core, pl.ds(lo, slabs[a] if size is None else size)]
        return pltpu.make_async_remote_copy(here, here, swap_send.at[a], share_recv.at[a], partner, MESH)

    def wait_all(here, sem):
        pltpu.make_async_copy(here, here, sem).wait()

    def grant(layer):
        pl.semaphore_signal(credit.at[layer], inc=1, device_id=behind[layer], device_id_type=MESH)

    def spend(layer):
        pl.semaphore_wait(credit.at[layer], 1)

    for layer in range(layers):
        prepare(0, layer).start()
    for layer in range(layers):
        first_own(0, layer).start()
    barrier = pltpu.get_barrier_semaphore()

    def greet(device):
        pl.semaphore_signal(barrier, inc=1, device_id=device, device_id_type=MESH)

    def answer(which, device):
        pl.semaphore_signal(entered.at[which], inc=1, device_id=device, device_id_type=MESH)

    def answer_chips():
        @pl.when(chip > 0)
        def _():
            answer(0, left)

        @pl.when(chip == last)
        def _():
            answer(1, right)

    greeted = jnp.where(chip > 0, 1, 0) + jnp.where(chip == last, 1, 0)
    pl.when(chip < last)(lambda: greet(right))
    pl.when(chip == 0)(lambda: greet(left))
    pl.when(core == 0)(lambda: greet(partner))
    for u in range(1, n + 1):
        for layer in range(layers):
            prepare(u, layer).start()

    @pl.when(core > 0)
    def _():
        pl.semaphore_wait(barrier, greeted + 1)
        answer(2, partner)
        answer_chips()

    @pl.when(core == 0)
    def _():
        pl.semaphore_wait(entered.at[2], 1)

    for u, (a, lo, size) in enumerate(units):
        wait_all(stage[a].at[:, pl.ds(lo, size)], stage_sem.at[u])
        for layer in range(layers):
            first_swap(u, layer).start()
        if u:
            for layer in range(layers):
                first_own(u, layer).start()
    for a, layer in pieces:
        swap(a, 1, layer, 0).start()

    @pl.when(core == 0)
    def _():
        @pl.when(chip > 0)
        def _():
            pl.semaphore_wait(barrier, greeted)

        answer_chips()

    def total(a, step, layer, i, arrived):
        t = own[a][step, layer, i].astype(jnp.float32) + pair[a][step, layer, i].astype(jnp.float32)
        if arrived is not None:
            t = t + ring[a][arrived, layer, i].astype(jnp.float32)
        return t

    def add(a, step, layer, arrived, lo, size):
        @pl.loop(lo, lo + size)
        def _(i):
            own[a][step, layer, i] = total(a, step, layer, i, arrived).astype(jnp.bfloat16)

    for u, (a, lo, size) in enumerate(units):
        wait_all(own[a].at[0, :, pl.ds(lo, size)], first_load.at[u])
        wait_all(pair[a].at[0, :, pl.ds(lo, size)], first_recv.at[u])
        for layer in range(layers):
            add(a, 0, layer, None, lo, size)

        def send(layer):
            if a < end:
                hop(a, 0, layer, lo, size).start()
                return
            hop(a, 0, layer, 0, split[layer]).start()

            @pl.when(chip != giver[layer])
            def _():
                hop(a, 0, layer, split[layer], whole - split[layer]).start()

            @pl.when(chip == giver[layer])
            def _():
                straight(layer).start()

        @pl.when(chip > 0)
        def _():
            send(1)

        if u == 0:

            @pl.when(chip < last)
            def _():
                pl.semaphore_wait(entered.at[0], 1)

        send(0)

    @pl.when(chip == 0)
    def _():
        pl.semaphore_wait(entered.at[1], 1)
        for a, lo, size in units:
            hop(a, 0, 1, lo, size).start()

    @pl.loop(1, chips)
    def _(step):
        for a, layer in pieces:
            load(a, step, layer).start()

    @pl.loop(2, chips)
    def _(step):
        for a, layer in pieces:
            swap(a, step, layer, 1).start()

    for a in range(n):
        pltpu.make_async_copy(m_in[a], new_m[a], load_sem.at[a]).start()
        pltpu.make_async_copy(v_in[a], new_v[a], load_sem.at[a]).start()
        for layer in range(layers):
            pltpu.make_async_copy(w[a].at[layer, chip, core], old_w[a].at[layer], load_sem.at[a]).start()
    for a in range(n):
        wait_all(new_w[a].at[:, pl.ds(0, (last + 1 + 4) // CORES)], load_sem.at[a])
        wait_all(pair[a].at[1], pair_recv.at[0, a])

    @pl.loop(1, last)
    def _(step):
        @pl.when(step == 2)
        def _():
            for a in range(n):
                wait_all(pair[a].at[pl.ds(2, chips - 2)], pair_recv.at[1, a])

        @pl.when(step >= SLOTS)
        def _():
            for layer in range(layers):
                spend(layer)

        for a, layer in pieces:
            if a == end:
                short = (step == 1) & (chip == 0)
                cut = split[layer]

                @pl.when(short)
                def _():
                    hop(a, 0, layer, 0, cut).wait_recv()
                    add(a, step, layer, None, cut, whole - cut)

                @pl.when(jnp.logical_not(short))
                def _():
                    hop(a, step - 1, layer).wait_recv()
                    add(a, step, layer, step - 1, cut, whole - cut)

                add(a, step, layer, step - 1, 0, cut)
            else:
                hop(a, step - 1, layer).wait_recv()
                add(a, step, layer, step - 1, 0, slabs[a])
            hop(a, step, layer).start()
            if a == end:
                grant(layer)

    def update(a, layer, lo, size, more=None):
        @pl.loop(lo, lo + size)
        def _(i):
            grad = total(a, last, layer, i, last - 1)
            if more is not None:
                grad = grad + more(i)
            grad = grad.astype(jnp.bfloat16).astype(jnp.float32)
            new = adamw(old_w[a][layer, i].astype(jnp.float32), new_m[a][layer, i], new_v[a][layer, i], grad)
            new_w[a][layer, chip, core, i], new_m[a][layer, i], new_v[a][layer, i] = new

    for layer in range(layers):
        spend(layer)
    for a, layer in pieces:
        hop(a, last - 1, layer).wait_recv()

        if a == end:
            cut = split[layer]
            update(a, layer, 0, cut)

            @pl.when(chip == taker[layer])
            def _():
                straight(layer).wait_recv()
                update(a, layer, cut, whole - cut, lambda i: extra[layer][i - cut].astype(jnp.float32))

            @pl.when(chip != taker[layer])
            def _():
                update(a, layer, cut, whole - cut)

        else:
            update(a, layer, 0, slabs[a])
        spread(a, 0, layer).start()
        share(a, 0, layer).start()
        if a == end:
            grant(layer)

            @pl.when(chip == sender[layer])
            def _():
                detour(layer).start()

    @pl.loop(1, last - 1)
    def _(step):
        for layer in range(layers):
            spend(layer)
        for a, layer in pieces:
            spread(a, step - 1, layer).wait_recv()
            spread(a, step, layer).start()
            share(a, step, layer).start()
            if a == end:

                @pl.when(step <= last - SLOTS)
                def _():
                    grant(layer)

    for layer in range(layers):
        spend(layer)
    for a, layer in pieces:
        spread(a, last - 2, layer).wait_recv()
        if a < end:
            spread(a, last - 1, layer).start()
        else:

            @pl.when(chip != keeper[layer])
            def _():
                spread_tail(last - 1, layer, 0).start()

            for k in range(1, PARTS + 1):
                spread_tail(last - 1, layer, k).start()
        share(a, last - 1, layer).start()

    for a in range(end):
        for layer in range(layers):
            spread(a, last - 1, layer).wait_recv()
            share(a, last, layer).start()
    for k in range(PARTS + 1):
        for layer in range(layers):
            spread_tail(last, layer, k).wait_recv()
            share(end, last, layer, *tail[layer][k]).start()

    for layer in range(layers):

        @pl.when(chip != keeper[layer])
        def _():
            spread_tail(last - 1, layer, 0).wait_send()

        @pl.when(chip == sender[layer])
        def _():
            detour(layer).wait_send()

        wait_all(new_w[end].at[layer, 0, 0, pl.ds(0, whole - DETOUR[layer])], tail_send.at[0, layer])
    for a in range(n):
        wait_all(new_w[a], swap_send.at[a])
        wait_all(new_w[a].at[:, pl.ds(0, last)] if a < end else ring[a], ring_send.at[a])
    wait_all(ring[end].at[pl.ds(0, last - 1)], gather_send)
    for a in range(n):
        wait_all(pair[a], share_recv.at[a])


def write(n, *refs):
    *refs, sem = refs
    sources, targets = refs[: 3 * n], refs[3 * n :]
    weights = list(zip(sources, targets, strict=True))[:n]
    for a, (source, target) in enumerate(weights):
        for layer in range(source.shape[0]):
            for chip in range(source.shape[1]):
                pltpu.make_async_copy(source.at[layer, chip], target.at[layer, chip], sem.at[a]).start()
    for source, target in zip(sources[n:], targets[n:], strict=True):
        pltpu.make_async_copy(source, target, sem.at[n]).start()
    for a, (source, target) in enumerate(weights):
        pltpu.make_async_copy(source, target, sem.at[a]).wait()
    part = sources[0].at[:, pl.ds(0, 2 * n)]
    pltpu.make_async_copy(part, part, sem.at[n]).wait()


def solution(mesh):
    chips = mesh.shape["dp"] // CORES

    def step(*arrays):
        terms, weights, m, v = (arrays[i : i + 3] for i in (0, 3, 6, 9))
        n, layers = len(terms), weights[0].shape[0]
        tiles = [(one.shape[1] // SUBLANES, SUBLANES, one.shape[2]) for one in m]
        whole = [(layers, chips, CORES, *tile) for tile in tiles]
        state = [(layers, *tile) for tile in tiles]
        operands = [one.reshape(shape) for one, shape in zip(terms, whole, strict=True)]
        operands += [one.reshape(shape) for one, shape in zip(weights, whole, strict=True)]
        operands += [one.reshape(shape) for part in (m, v) for one, shape in zip(part, state, strict=True)]
        sems = lambda *shape: pltpu.SemaphoreType.DMA(shape)
        vmem = lambda lead, dtype: [pltpu.VMEM((*lead, *tile), dtype) for tile in tiles]
        out = pl.pallas_call(
            functools.partial(kernel, n, chips, layers),
            out_shape=[pltpu.VMEM(shape, jnp.bfloat16) for shape in whole] + [pltpu.VMEM(shape, jnp.float32) for shape in state] * 2,
            in_specs=[pl.BlockSpec(memory_space=pl.ANY)] * len(operands),
            out_specs=[pl.BlockSpec(memory_space=pltpu.VMEM)] * (3 * n),
            scratch_shapes=[
                *vmem((chips, layers), jnp.bfloat16),
                *vmem((chips, layers), jnp.bfloat16),
                *vmem((chips - 1, layers), jnp.bfloat16),
                *vmem((layers,), jnp.bfloat16),
                *vmem((layers,), jnp.bfloat16),
                *[pltpu.VMEM((slabs, *tiles[-1][1:]), jnp.bfloat16) for slabs in (SEAM, LIFT)],
                sems(n + 1),
                sems(n + 1),
                sems(n),
                sems(n + 1),
                sems(2, n),
                sems(n, SLOTS, layers),
                sems(PARTS + 1, layers),
                sems(layers),
                sems(n),
                sems(n),
                sems(n),
                pltpu.SemaphoreType.DMA,
                sems(3, layers),
                pltpu.SemaphoreType.REGULAR((layers,)),
                pltpu.SemaphoreType.REGULAR((3,)),
            ],
            compiler_params=pltpu.CompilerParams(collective_id=0, has_side_effects=True, vmem_limit_bytes=40 << 20),
            name="step",
        )(*operands)
        out = pl.pallas_call(
            functools.partial(write, n),
            out_shape=[jax.ShapeDtypeStruct(one.shape, one.dtype) for one in out],
            in_specs=[pl.BlockSpec(memory_space=pltpu.VMEM)] * len(out),
            out_specs=[pl.BlockSpec(memory_space=pl.ANY)] * len(out),
            scratch_shapes=[sems(n + 1)],
            compiler_params=pltpu.CompilerParams(vmem_limit_bytes=1 << 20),
            name="write",
        )(*[pltpu.with_memory_space_constraint(one, pltpu.VMEM) for one in out])
        return tuple(one.reshape(like.shape) for one, like in zip(out, (*weights, *m, *v), strict=True))

    all_of, cut = P(None, None, None), P(None, "dp", None)
    return jax.shard_map(
        step,
        mesh=mesh,
        in_specs=(P(("rep", "dp"), None, None, None),) * 3 + (all_of,) * 3 + (cut,) * 6,
        out_specs=(P("rep", None, None),) * 3 + (P("rep", "dp", None),) * 6,
        check_vma=False,
    )
```

```python
import functools

import jax
import jax.numpy as jnp
from jax import lax
from jax.experimental import pallas as pl
from jax.experimental.pallas import tpu as pltpu
from jax.sharding import PartitionSpec as P

MESH = pl.DeviceIdType.MESH
CORES = 2
SUBLANES = 8
HEAD = 1
PARTS = 2
SEAM = 10
LIFT = 12
DETOUR = (12, 4)
SLOTS = 2


def adamw(w, m, v, g):
    m = 0.9 * m + 0.1 * g
    v = 0.95 * v + 0.05 * g * g
    step = m * lax.rsqrt(v + 1e-8) + 0.1 * w
    return (w - 0.02 * step).astype(jnp.bfloat16), m, v


def cuts(count, parts):
    edges = [count * i // parts for i in range(parts + 1)]
    return [(lo, hi - lo) for lo, hi in zip(edges, edges[1:])]


def kernel(n, chips, layers, *refs):
    refs = iter(refs)
    take = lambda count: [next(refs) for _ in range(count)]
    g, w, m_in, v_in = take(n), take(n), take(n), take(n)
    new_w, new_m, new_v = take(n), take(n), take(n)
    own, pair, ring, stage, old_w, extra = take(n), take(n), take(n), take(n), take(n), take(2)
    stage_sem, first_load, load_sem, first_recv, pair_recv, ring_recv, tail_recv, extra_recv, share_recv, swap_send, ring_send, gather_send, tail_send, credit, entered = take(15)

    me = lax.axis_index("dp")
    chip, core = me // CORES, me % CORES
    other = 1 - core
    last = chips - 1
    partner = {"dp": chip * CORES + other}
    right = {"dp": (chip + 1) % chips * CORES + core}
    left = {"dp": (chip + last) % chips * CORES + core}
    ahead = [left if layer % 2 else right for layer in range(layers)]
    behind = [right if layer % 2 else left for layer in range(layers)]
    slabs = [one.shape[2] for one in own]
    end = n - 1
    whole = slabs[end]
    giver, taker = (last, 1), (last - 1, 2)
    split = [whole - SEAM, whole - LIFT]
    pieces = [(a, layer) for a in range(n) for layer in range(layers)]
    units = [(0, 0, HEAD), (0, HEAD, slabs[0] - HEAD)] + [(a, 0, slabs[a]) for a in range(1, n)]

    def block(step, layer):
        return (chip + 1 + step if layer % 2 else chip + chips - 1 - step) % chips

    def source(step, layer):
        return (chip + step if layer % 2 else chip + chips - step) % chips

    def prepare(u, layer):
        a, lo, size = units[u]
        return pltpu.make_async_copy(
            g[a].at[layer, block(0, layer), other, pl.ds(lo, size)], stage[a].at[layer, pl.ds(lo, size)], stage_sem.at[u]
        )

    def first_own(u, layer):
        a, lo, size = units[u]
        return pltpu.make_async_copy(
            g[a].at[layer, block(0, layer), core, pl.ds(lo, size)], own[a].at[0, layer, pl.ds(lo, size)], first_load.at[u]
        )

    def first_swap(u, layer):
        a, lo, size = units[u]
        return pltpu.make_async_remote_copy(
            stage[a].at[layer, pl.ds(lo, size)], pair[a].at[0, layer, pl.ds(lo, size)], swap_send.at[a], first_recv.at[u], partner, MESH
        )

    def load(a, step, layer):
        return pltpu.make_async_copy(g[a].at[layer, block(step, layer), core], own[a].at[step, layer], load_sem.at[a])

    def swap(a, step, layer, sem):
        return pltpu.make_async_remote_copy(
            g[a].at[layer, block(step, layer), other], pair[a].at[step, layer], swap_send.at[a], pair_recv.at[sem, a], partner, MESH
        )

    def hop(a, step, layer, lo=0, size=None):
        part = pl.ds(lo, slabs[a] if size is None else size)
        return pltpu.make_async_remote_copy(
            own[a].at[step, layer, part],
            ring[a].at[step, layer, part],
            ring_send.at[a],
            ring_recv.at[a, step % SLOTS, layer],
            ahead[layer],
            MESH,
        )

    def spread(a, step, layer):
        here = new_w[a].at[layer, source(step, layer), core]
        return pltpu.make_async_remote_copy(
            here, here, ring_send.at[a] if a < end else gather_send, ring_recv.at[a, (step + last) % SLOTS, layer], ahead[layer], MESH
        )

    def straight(layer):
        part = pl.ds(split[layer], whole - split[layer])
        return pltpu.make_async_remote_copy(
            own[end].at[0, layer, part], extra[layer], ring_send.at[end], extra_recv.at[layer], behind[layer], MESH
        )

    sender, keeper = (1, last - 1), (last, 0)
    tail = [[(whole - skip, skip), *cuts(whole - skip, PARTS)] for skip in DETOUR]

    def spread_tail(step, layer, k):
        here = new_w[end].at[layer, source(step, layer), core, pl.ds(*tail[layer][k])]
        sem = tail_send.at[0 if k else 1, layer]
        return pltpu.make_async_remote_copy(here, here, sem, tail_recv.at[k, layer], ahead[layer], MESH)

    def detour(layer):
        here = new_w[end].at[layer, chip, core, pl.ds(*tail[layer][0])]
        return pltpu.make_async_remote_copy(here, here, tail_send.at[2, layer], tail_recv.at[0, layer], behind[layer], MESH)

    def share(a, step, layer, lo=0, size=None):
        here = new_w[a].at[layer, source(step, layer), core, pl.ds(lo, slabs[a] if size is None else size)]
        return pltpu.make_async_remote_copy(here, here, swap_send.at[a], share_recv.at[a], partner, MESH)

    def wait_all(here, sem):
        pltpu.make_async_copy(here, here, sem).wait()

    def grant(layer):
        pl.semaphore_signal(credit.at[layer], inc=1, device_id=behind[layer], device_id_type=MESH)

    def spend(layer):
        pl.semaphore_wait(credit.at[layer], 1)

    for layer in range(layers):
        prepare(0, layer).start()
    for layer in range(layers):
        first_own(0, layer).start()
    barrier = pltpu.get_barrier_semaphore()

    def greet(device):
        pl.semaphore_signal(barrier, inc=1, device_id=device, device_id_type=MESH)

    def answer(which, device):
        pl.semaphore_signal(entered.at[which], inc=1, device_id=device, device_id_type=MESH)

    def answer_chips():
        @pl.when(chip > 0)
        def _():
            answer(0, left)

        @pl.when(chip == last)
        def _():
            answer(1, right)

    greeted = jnp.where(chip > 0, 1, 0) + jnp.where(chip == last, 1, 0)
    pl.when(chip < last)(lambda: greet(right))
    pl.when(chip == 0)(lambda: greet(left))
    pl.when(core == 0)(lambda: greet(partner))
    for u in range(1, n + 1):
        for layer in range(layers):
            prepare(u, layer).start()

    @pl.when(core > 0)
    def _():
        pl.semaphore_wait(barrier, greeted + 1)
        answer(2, partner)
        answer_chips()

    @pl.when(core == 0)
    def _():
        pl.semaphore_wait(entered.at[2], 1)

    for u, (a, lo, size) in enumerate(units):
        wait_all(stage[a].at[:, pl.ds(lo, size)], stage_sem.at[u])
        for layer in range(layers):
            first_swap(u, layer).start()
        if u:
            for layer in range(layers):
                first_own(u, layer).start()
    for a, layer in pieces:
        swap(a, 1, layer, 0).start()

    @pl.when(core == 0)
    def _():
        @pl.when(chip > 0)
        def _():
            pl.semaphore_wait(barrier, greeted)

        answer_chips()

    def total(a, step, layer, i, arrived):
        t = own[a][step, layer, i].astype(jnp.float32) + pair[a][step, layer, i].astype(jnp.float32)
        if arrived is not None:
            t = t + ring[a][arrived, layer, i].astype(jnp.float32)
        return t

    def add(a, step, layer, arrived, lo, size):
        @pl.loop(lo, lo + size)
        def _(i):
            own[a][step, layer, i] = total(a, step, layer, i, arrived).astype(jnp.bfloat16)

    for u, (a, lo, size) in enumerate(units):
        wait_all(own[a].at[0, :, pl.ds(lo, size)], first_load.at[u])
        wait_all(pair[a].at[0, :, pl.ds(lo, size)], first_recv.at[u])
        for layer in range(layers):
            add(a, 0, layer, None, lo, size)

        def send(layer):
            if a < end:
                hop(a, 0, layer, lo, size).start()
                return
            hop(a, 0, layer, 0, split[layer]).start()

            @pl.when(chip != giver[layer])
            def _():
                hop(a, 0, layer, split[layer], whole - split[layer]).start()

            @pl.when(chip == giver[layer])
            def _():
                straight(layer).start()

        @pl.when(chip > 0)
        def _():
            send(1)

        if u == 0:

            @pl.when(chip < last)
            def _():
                pl.semaphore_wait(entered.at[0], 1)

        send(0)

    @pl.when(chip == 0)
    def _():
        pl.semaphore_wait(entered.at[1], 1)
        for a, lo, size in units:
            hop(a, 0, 1, lo, size).start()

    @pl.loop(1, chips)
    def _(step):
        for a, layer in pieces:
            load(a, step, layer).start()

    @pl.loop(2, chips)
    def _(step):
        for a, layer in pieces:
            swap(a, step, layer, 1).start()

    for a in range(n):
        pltpu.make_async_copy(m_in[a], new_m[a], load_sem.at[a]).start()
        pltpu.make_async_copy(v_in[a], new_v[a], load_sem.at[a]).start()
        for layer in range(layers):
            pltpu.make_async_copy(w[a].at[layer, chip, core], old_w[a].at[layer], load_sem.at[a]).start()
    for a in range(n):
        wait_all(new_w[a].at[:, pl.ds(0, (last + 1 + 4) // CORES)], load_sem.at[a])
        wait_all(pair[a].at[1], pair_recv.at[0, a])

    @pl.loop(1, last)
    def _(step):
        @pl.when(step == 2)
        def _():
            for a in range(n):
                wait_all(pair[a].at[pl.ds(2, chips - 2)], pair_recv.at[1, a])

        @pl.when(step >= SLOTS)
        def _():
            for layer in range(layers):
                spend(layer)

        for a, layer in pieces:
            if a == end:
                short = (step == 1) & (chip == 0)
                cut = split[layer]

                @pl.when(short)
                def _():
                    hop(a, 0, layer, 0, cut).wait_recv()
                    add(a, step, layer, None, cut, whole - cut)

                @pl.when(jnp.logical_not(short))
                def _():
                    hop(a, step - 1, layer).wait_recv()
                    add(a, step, layer, step - 1, cut, whole - cut)

                add(a, step, layer, step - 1, 0, cut)
            else:
                hop(a, step - 1, layer).wait_recv()
                add(a, step, layer, step - 1, 0, slabs[a])
            hop(a, step, layer).start()
            if a == end:
                grant(layer)

    def update(a, layer, lo, size, more=None):
        @pl.loop(lo, lo + size)
        def _(i):
            grad = total(a, last, layer, i, last - 1)
            if more is not None:
                grad = grad + more(i)
            grad = grad.astype(jnp.bfloat16).astype(jnp.float32)
            new = adamw(old_w[a][layer, i].astype(jnp.float32), new_m[a][layer, i], new_v[a][layer, i], grad)
            new_w[a][layer, chip, core, i], new_m[a][layer, i], new_v[a][layer, i] = new

    for layer in range(layers):
        spend(layer)
    for a, layer in pieces:
        hop(a, last - 1, layer).wait_recv()

        if a == end:
            cut = split[layer]
            update(a, layer, 0, cut)

            @pl.when(chip == taker[layer])
            def _():
                straight(layer).wait_recv()
                update(a, layer, cut, whole - cut, lambda i: extra[layer][i - cut].astype(jnp.float32))

            @pl.when(chip != taker[layer])
            def _():
                update(a, layer, cut, whole - cut)

        else:
            update(a, layer, 0, slabs[a])
        spread(a, 0, layer).start()
        share(a, 0, layer).start()
        if a == end:
            grant(layer)

            @pl.when(chip == sender[layer])
            def _():
                detour(layer).start()

    @pl.loop(1, last - 1)
    def _(step):
        for layer in range(layers):
            spend(layer)
        for a, layer in pieces:
            spread(a, step - 1, layer).wait_recv()
            spread(a, step, layer).start()
            share(a, step, layer).start()
            if a == end:

                @pl.when(step <= last - SLOTS)
                def _():
                    grant(layer)

    for layer in range(layers):
        spend(layer)
    for a, layer in pieces:
        spread(a, last - 2, layer).wait_recv()
        if a < end:
            spread(a, last - 1, layer).start()
        else:

            @pl.when(chip != keeper[layer])
            def _():
                spread_tail(last - 1, layer, 0).start()

            for k in range(1, PARTS + 1):
                spread_tail(last - 1, layer, k).start()
        share(a, last - 1, layer).start()

    for a in range(end):
        for layer in range(layers):
            spread(a, last - 1, layer).wait_recv()
            share(a, last, layer).start()
    for k in range(PARTS + 1):
        for layer in range(layers):
            spread_tail(last, layer, k).wait_recv()
            share(end, last, layer, *tail[layer][k]).start()

    for layer in range(layers):

        @pl.when(chip != keeper[layer])
        def _():
            spread_tail(last - 1, layer, 0).wait_send()

        @pl.when(chip == sender[layer])
        def _():
            detour(layer).wait_send()

        wait_all(new_w[end].at[layer, 0, 0, pl.ds(0, whole - DETOUR[layer])], tail_send.at[0, layer])
    for a in range(n):
        wait_all(new_w[a], swap_send.at[a])
        wait_all(new_w[a].at[:, pl.ds(0, last)] if a < end else ring[a], ring_send.at[a])
    wait_all(ring[end].at[pl.ds(0, last - 1)], gather_send)
    for a in range(n):
        wait_all(pair[a], share_recv.at[a])


def write(n, *refs):
    *refs, sem = refs
    sources, targets = refs[: 3 * n], refs[3 * n :]
    weights = list(zip(sources, targets, strict=True))[:n]
    for a, (source, target) in enumerate(weights):
        for layer in range(source.shape[0]):
            for chip in range(source.shape[1]):
                pltpu.make_async_copy(source.at[layer, chip], target.at[layer, chip], sem.at[a]).start()
    for source, target in zip(sources[n:], targets[n:], strict=True):
        pltpu.make_async_copy(source, target, sem.at[n]).start()
    for a, (source, target) in enumerate(weights):
        pltpu.make_async_copy(source, target, sem.at[a]).wait()
    part = sources[0].at[:, pl.ds(0, 2 * n)]
    pltpu.make_async_copy(part, part, sem.at[n]).wait()


def solution(mesh):
    chips = mesh.shape["dp"] // CORES

    def step(*arrays):
        terms, weights, m, v = (arrays[i : i + 3] for i in (0, 3, 6, 9))
        n, layers = len(terms), weights[0].shape[0]
        tiles = [(one.shape[1] // SUBLANES, SUBLANES, one.shape[2]) for one in m]
        whole = [(layers, chips, CORES, *tile) for tile in tiles]
        state = [(layers, *tile) for tile in tiles]
        operands = [one.reshape(shape) for one, shape in zip(terms, whole, strict=True)]
        operands += [one.reshape(shape) for one, shape in zip(weights, whole, strict=True)]
        operands += [one.reshape(shape) for part in (m, v) for one, shape in zip(part, state, strict=True)]
        sems = lambda *shape: pltpu.SemaphoreType.DMA(shape)
        vmem = lambda lead, dtype: [pltpu.VMEM((*lead, *tile), dtype) for tile in tiles]
        out = pl.pallas_call(
            functools.partial(kernel, n, chips, layers),
            out_shape=[pltpu.VMEM(shape, jnp.bfloat16) for shape in whole] + [pltpu.VMEM(shape, jnp.float32) for shape in state] * 2,
            in_specs=[pl.BlockSpec(memory_space=pl.ANY)] * len(operands),
            out_specs=[pl.BlockSpec(memory_space=pltpu.VMEM)] * (3 * n),
            scratch_shapes=[
                *vmem((chips, layers), jnp.bfloat16),
                *vmem((chips, layers), jnp.bfloat16),
                *vmem((chips - 1, layers), jnp.bfloat16),
                *vmem((layers,), jnp.bfloat16),
                *vmem((layers,), jnp.bfloat16),
                *[pltpu.VMEM((slabs, *tiles[-1][1:]), jnp.bfloat16) for slabs in (SEAM, LIFT)],
                sems(n + 1),
                sems(n + 1),
                sems(n),
                sems(n + 1),
                sems(2, n),
                sems(n, SLOTS, layers),
                sems(PARTS + 1, layers),
                sems(layers),
                sems(n),
                sems(n),
                sems(n),
                pltpu.SemaphoreType.DMA,
                sems(3, layers),
                pltpu.SemaphoreType.REGULAR((layers,)),
                pltpu.SemaphoreType.REGULAR((3,)),
            ],
            compiler_params=pltpu.CompilerParams(collective_id=0, has_side_effects=True, vmem_limit_bytes=40 << 20),
            name="step",
        )(*operands)
        out = pl.pallas_call(
            functools.partial(write, n),
            out_shape=[jax.ShapeDtypeStruct(one.shape, one.dtype) for one in out],
            in_specs=[pl.BlockSpec(memory_space=pltpu.VMEM)] * len(out),
            out_specs=[pl.BlockSpec(memory_space=pl.ANY)] * len(out),
            scratch_shapes=[sems(n + 1)],
            compiler_params=pltpu.CompilerParams(vmem_limit_bytes=1 << 20),
            name="write",
        )(*[pltpu.with_memory_space_constraint(one, pltpu.VMEM) for one in out])
        return tuple(one.reshape(like.shape) for one, like in zip(out, (*weights, *m, *v), strict=True))

    all_of, cut = P(None, None, None), P(None, "dp", None)
    return jax.shard_map(
        step,
        mesh=mesh,
        in_specs=(P(("rep", "dp"), None, None, None),) * 3 + (all_of,) * 3 + (cut,) * 6,
        out_specs=(P("rep", None, None),) * 3 + (P("rep", "dp", None),) * 6,
        check_vma=False,
    )
```

```python
import functools

import jax
import jax.numpy as jnp
from jax import lax
from jax.experimental import pallas as pl
from jax.experimental.pallas import tpu as pltpu
from jax.sharding import PartitionSpec as P

MESH = pl.DeviceIdType.MESH
CORES = 2
SUBLANES = 8
HEAD = 1
PARTS = 2
SEAM = 10
LIFT = 12
DETOUR = (12, 4)
SLOTS = 2


def adamw(w, m, v, g):
    m = 0.9 * m + 0.1 * g
    v = 0.95 * v + 0.05 * g * g
    step = m * lax.rsqrt(v + 1e-8) + 0.1 * w
    return (w - 0.02 * step).astype(jnp.bfloat16), m, v


def cuts(count, parts):
    edges = [count * i // parts for i in range(parts + 1)]
    return [(lo, hi - lo) for lo, hi in zip(edges, edges[1:])]


def kernel(n, chips, layers, *refs):
    refs = iter(refs)
    take = lambda count: [next(refs) for _ in range(count)]
    g, w, m_in, v_in = take(n), take(n), take(n), take(n)
    new_w, new_m, new_v = take(n), take(n), take(n)
    own, pair, ring, stage, old_w, extra = take(n), take(n), take(n), take(n), take(n), take(2)
    stage_sem, first_load, load_sem, first_recv, pair_recv, ring_recv, tail_recv, extra_recv, share_recv, swap_send, ring_send, gather_send, tail_send, credit, entered = take(15)

    me = lax.axis_index("dp")
    chip, core = me // CORES, me % CORES
    other = 1 - core
    last = chips - 1
    partner = {"dp": chip * CORES + other}
    right = {"dp": (chip + 1) % chips * CORES + core}
    left = {"dp": (chip + last) % chips * CORES + core}
    ahead = [left if layer % 2 else right for layer in range(layers)]
    behind = [right if layer % 2 else left for layer in range(layers)]
    slabs = [one.shape[2] for one in own]
    end = n - 1
    whole = slabs[end]
    giver, taker = (last, 1), (last - 1, 2)
    split = [whole - SEAM, whole - LIFT]
    pieces = [(a, layer) for a in range(n) for layer in range(layers)]
    units = [(0, 0, HEAD), (0, HEAD, slabs[0] - HEAD)] + [(a, 0, slabs[a]) for a in range(1, n)]

    def block(step, layer):
        return (chip + 1 + step if layer % 2 else chip + chips - 1 - step) % chips

    def source(step, layer):
        return (chip + step if layer % 2 else chip + chips - step) % chips

    def prepare(u, layer):
        a, lo, size = units[u]
        return pltpu.make_async_copy(
            g[a].at[layer, block(0, layer), other, pl.ds(lo, size)], stage[a].at[layer, pl.ds(lo, size)], stage_sem.at[u]
        )

    def first_own(u, layer):
        a, lo, size = units[u]
        return pltpu.make_async_copy(
            g[a].at[layer, block(0, layer), core, pl.ds(lo, size)], own[a].at[0, layer, pl.ds(lo, size)], first_load.at[u]
        )

    def first_swap(u, layer):
        a, lo, size = units[u]
        return pltpu.make_async_remote_copy(
            stage[a].at[layer, pl.ds(lo, size)], pair[a].at[0, layer, pl.ds(lo, size)], swap_send.at[a], first_recv.at[u], partner, MESH
        )

    def load(a, step, layer):
        return pltpu.make_async_copy(g[a].at[layer, block(step, layer), core], own[a].at[step, layer], load_sem.at[a])

    def swap(a, step, layer, sem):
        return pltpu.make_async_remote_copy(
            g[a].at[layer, block(step, layer), other], pair[a].at[step, layer], swap_send.at[a], pair_recv.at[sem, a], partner, MESH
        )

    def hop(a, step, layer, lo=0, size=None):
        part = pl.ds(lo, slabs[a] if size is None else size)
        return pltpu.make_async_remote_copy(
            own[a].at[step, layer, part],
            ring[a].at[step, layer, part],
            ring_send.at[a],
            ring_recv.at[a, step % SLOTS, layer],
            ahead[layer],
            MESH,
        )

    def spread(a, step, layer):
        here = new_w[a].at[layer, source(step, layer), core]
        return pltpu.make_async_remote_copy(
            here, here, ring_send.at[a] if a < end else gather_send, ring_recv.at[a, (step + last) % SLOTS, layer], ahead[layer], MESH
        )

    def straight(layer):
        part = pl.ds(split[layer], whole - split[layer])
        return pltpu.make_async_remote_copy(
            own[end].at[0, layer, part], extra[layer], ring_send.at[end], extra_recv.at[layer], behind[layer], MESH
        )

    sender, keeper = (1, last - 1), (last, 0)
    tail = [[(whole - skip, skip), *cuts(whole - skip, PARTS)] for skip in DETOUR]

    def spread_tail(step, layer, k):
        here = new_w[end].at[layer, source(step, layer), core, pl.ds(*tail[layer][k])]
        sem = tail_send.at[0 if k else 1, layer]
        return pltpu.make_async_remote_copy(here, here, sem, tail_recv.at[k, layer], ahead[layer], MESH)

    def detour(layer):
        here = new_w[end].at[layer, chip, core, pl.ds(*tail[layer][0])]
        return pltpu.make_async_remote_copy(here, here, tail_send.at[2, layer], tail_recv.at[0, layer], behind[layer], MESH)

    def share(a, step, layer, lo=0, size=None):
        here = new_w[a].at[layer, source(step, layer), core, pl.ds(lo, slabs[a] if size is None else size)]
        return pltpu.make_async_remote_copy(here, here, swap_send.at[a], share_recv.at[a], partner, MESH)

    def wait_all(here, sem):
        pltpu.make_async_copy(here, here, sem).wait()

    def grant(layer):
        pl.semaphore_signal(credit.at[layer], inc=1, device_id=behind[layer], device_id_type=MESH)

    def spend(layer):
        pl.semaphore_wait(credit.at[layer], 1)

    for layer in range(layers):
        prepare(0, layer).start()
    for layer in range(layers):
        first_own(0, layer).start()
    barrier = pltpu.get_barrier_semaphore()

    def greet(device):
        pl.semaphore_signal(barrier, inc=1, device_id=device, device_id_type=MESH)

    def answer(which, device):
        pl.semaphore_signal(entered.at[which], inc=1, device_id=device, device_id_type=MESH)

    def answer_chips():
        @pl.when(chip > 0)
        def _():
            answer(0, left)

        @pl.when(chip == last)
        def _():
            answer(1, right)

    greeted = jnp.where(chip > 0, 1, 0) + jnp.where(chip == last, 1, 0)
    pl.when(chip < last)(lambda: greet(right))
    pl.when(chip == 0)(lambda: greet(left))
    pl.when(core == 0)(lambda: greet(partner))
    for u in range(1, n + 1):
        for layer in range(layers):
            prepare(u, layer).start()

    @pl.when(core > 0)
    def _():
        pl.semaphore_wait(barrier, greeted + 1)
        answer(2, partner)
        answer_chips()

    @pl.when(core == 0)
    def _():
        pl.semaphore_wait(entered.at[2], 1)

    for u, (a, lo, size) in enumerate(units):
        wait_all(stage[a].at[:, pl.ds(lo, size)], stage_sem.at[u])
        for layer in range(layers):
            first_swap(u, layer).start()
        if u:
            for layer in range(layers):
                first_own(u, layer).start()
    for a, layer in pieces:
        swap(a, 1, layer, 0).start()

    @pl.when(core == 0)
    def _():
        @pl.when(chip > 0)
        def _():
            pl.semaphore_wait(barrier, greeted)

        answer_chips()

    def total(a, step, layer, i, arrived):
        t = own[a][step, layer, i].astype(jnp.float32) + pair[a][step, layer, i].astype(jnp.float32)
        if arrived is not None:
            t = t + ring[a][arrived, layer, i].astype(jnp.float32)
        return t

    def add(a, step, layer, arrived, lo, size):
        @pl.loop(lo, lo + size)
        def _(i):
            own[a][step, layer, i] = total(a, step, layer, i, arrived).astype(jnp.bfloat16)

    for u, (a, lo, size) in enumerate(units):
        wait_all(own[a].at[0, :, pl.ds(lo, size)], first_load.at[u])
        wait_all(pair[a].at[0, :, pl.ds(lo, size)], first_recv.at[u])
        for layer in range(layers):
            add(a, 0, layer, None, lo, size)

        def send(layer):
            if a < end:
                hop(a, 0, layer, lo, size).start()
                return
            hop(a, 0, layer, 0, split[layer]).start()

            @pl.when(chip != giver[layer])
            def _():
                hop(a, 0, layer, split[layer], whole - split[layer]).start()

            @pl.when(chip == giver[layer])
            def _():
                straight(layer).start()

        @pl.when(chip > 0)
        def _():
            send(1)

        if u == 0:

            @pl.when(chip < last)
            def _():
                pl.semaphore_wait(entered.at[0], 1)

        send(0)

    @pl.when(chip == 0)
    def _():
        pl.semaphore_wait(entered.at[1], 1)
        for a, lo, size in units:
            hop(a, 0, 1, lo, size).start()

    @pl.loop(1, chips)
    def _(step):
        for a, layer in pieces:
            load(a, step, layer).start()

    @pl.loop(2, chips)
    def _(step):
        for a, layer in pieces:
            swap(a, step, layer, 1).start()

    for a in range(n):
        pltpu.make_async_copy(m_in[a], new_m[a], load_sem.at[a]).start()
        pltpu.make_async_copy(v_in[a], new_v[a], load_sem.at[a]).start()
        for layer in range(layers):
            pltpu.make_async_copy(w[a].at[layer, chip, core], old_w[a].at[layer], load_sem.at[a]).start()
    for a in range(n):
        wait_all(new_w[a].at[:, pl.ds(0, (last + 1 + 4) // CORES)], load_sem.at[a])
        wait_all(pair[a].at[1], pair_recv.at[0, a])

    @pl.loop(1, last)
    def _(step):
        @pl.when(step == 2)
        def _():
            for a in range(n):
                wait_all(pair[a].at[pl.ds(2, chips - 2)], pair_recv.at[1, a])

        @pl.when(step >= SLOTS)
        def _():
            for layer in range(layers):
                spend(layer)

        for a, layer in pieces:
            if a == end:
                short = (step == 1) & (chip == 0)
                cut = split[layer]

                @pl.when(short)
                def _():
                    hop(a, 0, layer, 0, cut).wait_recv()
                    add(a, step, layer, None, cut, whole - cut)

                @pl.when(jnp.logical_not(short))
                def _():
                    hop(a, step - 1, layer).wait_recv()
                    add(a, step, layer, step - 1, cut, whole - cut)

                add(a, step, layer, step - 1, 0, cut)
            else:
                hop(a, step - 1, layer).wait_recv()
                add(a, step, layer, step - 1, 0, slabs[a])
            hop(a, step, layer).start()
            if a == end:
                grant(layer)

    def update(a, layer, lo, size, more=None):
        @pl.loop(lo, lo + size)
        def _(i):
            grad = total(a, last, layer, i, last - 1)
            if more is not None:
                grad = grad + more(i)
            grad = grad.astype(jnp.bfloat16).astype(jnp.float32)
            new = adamw(old_w[a][layer, i].astype(jnp.float32), new_m[a][layer, i], new_v[a][layer, i], grad)
            new_w[a][layer, chip, core, i], new_m[a][layer, i], new_v[a][layer, i] = new

    for layer in range(layers):
        spend(layer)
    for a, layer in pieces:
        hop(a, last - 1, layer).wait_recv()

        if a == end:
            cut = split[layer]
            update(a, layer, 0, cut)

            @pl.when(chip == taker[layer])
            def _():
                straight(layer).wait_recv()
                update(a, layer, cut, whole - cut, lambda i: extra[layer][i - cut].astype(jnp.float32))

            @pl.when(chip != taker[layer])
            def _():
                update(a, layer, cut, whole - cut)

        else:
            update(a, layer, 0, slabs[a])
        spread(a, 0, layer).start()
        share(a, 0, layer).start()
        if a == end:
            grant(layer)

            @pl.when(chip == sender[layer])
            def _():
                detour(layer).start()

    @pl.loop(1, last - 1)
    def _(step):
        for layer in range(layers):
            spend(layer)
        for a, layer in pieces:
            spread(a, step - 1, layer).wait_recv()
            spread(a, step, layer).start()
            share(a, step, layer).start()
            if a == end:

                @pl.when(step <= last - SLOTS)
                def _():
                    grant(layer)

    for layer in range(layers):
        spend(layer)
    for a, layer in pieces:
        spread(a, last - 2, layer).wait_recv()
        if a < end:
            spread(a, last - 1, layer).start()
        else:

            @pl.when(chip != keeper[layer])
            def _():
                spread_tail(last - 1, layer, 0).start()

            for k in range(1, PARTS + 1):
                spread_tail(last - 1, layer, k).start()
        share(a, last - 1, layer).start()

    for a in range(end):
        for layer in range(layers):
            spread(a, last - 1, layer).wait_recv()
            share(a, last, layer).start()
    for k in range(PARTS + 1):
        for layer in range(layers):
            spread_tail(last, layer, k).wait_recv()
            share(end, last, layer, *tail[layer][k]).start()

    for layer in range(layers):

        @pl.when(chip != keeper[layer])
        def _():
            spread_tail(last - 1, layer, 0).wait_send()

        @pl.when(chip == sender[layer])
        def _():
            detour(layer).wait_send()

        wait_all(new_w[end].at[layer, 0, 0, pl.ds(0, whole - DETOUR[layer])], tail_send.at[0, layer])
    for a in range(n):
        wait_all(new_w[a], swap_send.at[a])
        wait_all(new_w[a].at[:, pl.ds(0, last)] if a < end else ring[a], ring_send.at[a])
    wait_all(ring[end].at[pl.ds(0, last - 1)], gather_send)
    for a in range(n):
        wait_all(pair[a], share_recv.at[a])


def write(n, *refs):
    *refs, sem = refs
    sources, targets = refs[: 3 * n], refs[3 * n :]
    weights = list(zip(sources, targets, strict=True))[:n]
    for a, (source, target) in enumerate(weights):
        for layer in range(source.shape[0]):
            for chip in range(source.shape[1]):
                for core in range(source.shape[2]):
                    pltpu.make_async_copy(source.at[layer, chip, core], target.at[layer, chip, core], sem.at[a]).start()
    for source, target in zip(sources[n:], targets[n:], strict=True):
        pltpu.make_async_copy(source, target, sem.at[n]).start()
    for a, (source, target) in enumerate(weights):
        pltpu.make_async_copy(source, target, sem.at[a]).wait()
    part = sources[0].at[:, pl.ds(0, 2 * n)]
    pltpu.make_async_copy(part, part, sem.at[n]).wait()


def solution(mesh):
    chips = mesh.shape["dp"] // CORES

    def step(*arrays):
        terms, weights, m, v = (arrays[i : i + 3] for i in (0, 3, 6, 9))
        n, layers = len(terms), weights[0].shape[0]
        tiles = [(one.shape[1] // SUBLANES, SUBLANES, one.shape[2]) for one in m]
        whole = [(layers, chips, CORES, *tile) for tile in tiles]
        state = [(layers, *tile) for tile in tiles]
        operands = [one.reshape(shape) for one, shape in zip(terms, whole, strict=True)]
        operands += [one.reshape(shape) for one, shape in zip(weights, whole, strict=True)]
        operands += [one.reshape(shape) for part in (m, v) for one, shape in zip(part, state, strict=True)]
        sems = lambda *shape: pltpu.SemaphoreType.DMA(shape)
        vmem = lambda lead, dtype: [pltpu.VMEM((*lead, *tile), dtype) for tile in tiles]
        out = pl.pallas_call(
            functools.partial(kernel, n, chips, layers),
            out_shape=[pltpu.VMEM(shape, jnp.bfloat16) for shape in whole] + [pltpu.VMEM(shape, jnp.float32) for shape in state] * 2,
            in_specs=[pl.BlockSpec(memory_space=pl.ANY)] * len(operands),
            out_specs=[pl.BlockSpec(memory_space=pltpu.VMEM)] * (3 * n),
            scratch_shapes=[
                *vmem((chips, layers), jnp.bfloat16),
                *vmem((chips, layers), jnp.bfloat16),
                *vmem((chips - 1, layers), jnp.bfloat16),
                *vmem((layers,), jnp.bfloat16),
                *vmem((layers,), jnp.bfloat16),
                *[pltpu.VMEM((slabs, *tiles[-1][1:]), jnp.bfloat16) for slabs in (SEAM, LIFT)],
                sems(n + 1),
                sems(n + 1),
                sems(n),
                sems(n + 1),
                sems(2, n),
                sems(n, SLOTS, layers),
                sems(PARTS + 1, layers),
                sems(layers),
                sems(n),
                sems(n),
                sems(n),
                pltpu.SemaphoreType.DMA,
                sems(3, layers),
                pltpu.SemaphoreType.REGULAR((layers,)),
                pltpu.SemaphoreType.REGULAR((3,)),
            ],
            compiler_params=pltpu.CompilerParams(collective_id=0, has_side_effects=True, vmem_limit_bytes=40 << 20),
            name="step",
        )(*operands)
        out = pl.pallas_call(
            functools.partial(write, n),
            out_shape=[jax.ShapeDtypeStruct(one.shape, one.dtype) for one in out],
            in_specs=[pl.BlockSpec(memory_space=pltpu.VMEM)] * len(out),
            out_specs=[pl.BlockSpec(memory_space=pl.ANY)] * len(out),
            scratch_shapes=[sems(n + 1)],
            compiler_params=pltpu.CompilerParams(vmem_limit_bytes=1 << 20),
            name="write",
        )(*[pltpu.with_memory_space_constraint(one, pltpu.VMEM) for one in out])
        return tuple(one.reshape(like.shape) for one, like in zip(out, (*weights, *m, *v), strict=True))

    all_of, cut = P(None, None, None), P(None, "dp", None)
    return jax.shard_map(
        step,
        mesh=mesh,
        in_specs=(P(("rep", "dp"), None, None, None),) * 3 + (all_of,) * 3 + (cut,) * 6,
        out_specs=(P("rep", None, None),) * 3 + (P("rep", "dp", None),) * 6,
        check_vma=False,
    )
```

```python
import functools

import jax
import jax.numpy as jnp
from jax import lax
from jax.experimental import pallas as pl
from jax.experimental.pallas import tpu as pltpu
from jax.sharding import PartitionSpec as P

MESH = pl.DeviceIdType.MESH
CORES = 2
SUBLANES = 8
HEAD = 1
PARTS = 3
SEAM = 10
LIFT = 12
DETOUR = (12, 4)
SLOTS = 2


def adamw(w, m, v, g):
    m = 0.9 * m + 0.1 * g
    v = 0.95 * v + 0.05 * g * g
    step = m * lax.rsqrt(v + 1e-8) + 0.1 * w
    return (w - 0.02 * step).astype(jnp.bfloat16), m, v


def cuts(count, parts):
    edges = [count * i // parts for i in range(parts + 1)]
    return [(lo, hi - lo) for lo, hi in zip(edges, edges[1:])]


def kernel(n, chips, layers, *refs):
    refs = iter(refs)
    take = lambda count: [next(refs) for _ in range(count)]
    g, w, m_in, v_in = take(n), take(n), take(n), take(n)
    new_w, new_m, new_v = take(n), take(n), take(n)
    own, pair, ring, stage, old_w, extra = take(n), take(n), take(n), take(n), take(n), take(2)
    stage_sem, first_load, load_sem, first_recv, pair_recv, ring_recv, tail_recv, extra_recv, share_recv, swap_send, ring_send, gather_send, tail_send, credit, entered = take(15)

    me = lax.axis_index("dp")
    chip, core = me // CORES, me % CORES
    other = 1 - core
    last = chips - 1
    partner = {"dp": chip * CORES + other}
    right = {"dp": (chip + 1) % chips * CORES + core}
    left = {"dp": (chip + last) % chips * CORES + core}
    ahead = [left if layer % 2 else right for layer in range(layers)]
    behind = [right if layer % 2 else left for layer in range(layers)]
    slabs = [one.shape[2] for one in own]
    end = n - 1
    whole = slabs[end]
    giver, taker = (last, 1), (last - 1, 2)
    split = [whole - SEAM, whole - LIFT]
    pieces = [(a, layer) for a in range(n) for layer in range(layers)]
    units = [(0, 0, HEAD), (0, HEAD, slabs[0] - HEAD)] + [(a, 0, slabs[a]) for a in range(1, n)]

    def block(step, layer):
        return (chip + 1 + step if layer % 2 else chip + chips - 1 - step) % chips

    def source(step, layer):
        return (chip + step if layer % 2 else chip + chips - step) % chips

    def prepare(u, layer):
        a, lo, size = units[u]
        return pltpu.make_async_copy(
            g[a].at[layer, block(0, layer), other, pl.ds(lo, size)], stage[a].at[layer, pl.ds(lo, size)], stage_sem.at[u]
        )

    def first_own(u, layer):
        a, lo, size = units[u]
        return pltpu.make_async_copy(
            g[a].at[layer, block(0, layer), core, pl.ds(lo, size)], own[a].at[0, layer, pl.ds(lo, size)], first_load.at[u]
        )

    def first_swap(u, layer):
        a, lo, size = units[u]
        return pltpu.make_async_remote_copy(
            stage[a].at[layer, pl.ds(lo, size)], pair[a].at[0, layer, pl.ds(lo, size)], swap_send.at[a], first_recv.at[u], partner, MESH
        )

    def load(a, step, layer):
        return pltpu.make_async_copy(g[a].at[layer, block(step, layer), core], own[a].at[step, layer], load_sem.at[a])

    def swap(a, step, layer, sem):
        return pltpu.make_async_remote_copy(
            g[a].at[layer, block(step, layer), other], pair[a].at[step, layer], swap_send.at[a], pair_recv.at[sem, a], partner, MESH
        )

    def hop(a, step, layer, lo=0, size=None):
        part = pl.ds(lo, slabs[a] if size is None else size)
        return pltpu.make_async_remote_copy(
            own[a].at[step, layer, part],
            ring[a].at[step, layer, part],
            ring_send.at[a],
            ring_recv.at[a, step % SLOTS, layer],
            ahead[layer],
            MESH,
        )

    def spread(a, step, layer):
        here = new_w[a].at[layer, source(step, layer), core]
        return pltpu.make_async_remote_copy(
            here, here, ring_send.at[a] if a < end else gather_send, ring_recv.at[a, (step + last) % SLOTS, layer], ahead[layer], MESH
        )

    def straight(layer):
        part = pl.ds(split[layer], whole - split[layer])
        return pltpu.make_async_remote_copy(
            own[end].at[0, layer, part], extra[layer], ring_send.at[end], extra_recv.at[layer], behind[layer], MESH
        )

    sender, keeper = (1, last - 1), (last, 0)
    tail = [[(whole - skip, skip), *cuts(whole - skip, PARTS)] for skip in DETOUR]

    def spread_tail(step, layer, k):
        here = new_w[end].at[layer, source(step, layer), core, pl.ds(*tail[layer][k])]
        sem = tail_send.at[0 if k else 1, layer]
        return pltpu.make_async_remote_copy(here, here, sem, tail_recv.at[k, layer], ahead[layer], MESH)

    def detour(layer):
        here = new_w[end].at[layer, chip, core, pl.ds(*tail[layer][0])]
        return pltpu.make_async_remote_copy(here, here, tail_send.at[2, layer], tail_recv.at[0, layer], behind[layer], MESH)

    def share(a, step, layer, lo=0, size=None):
        here = new_w[a].at[layer, source(step, layer), core, pl.ds(lo, slabs[a] if size is None else size)]
        return pltpu.make_async_remote_copy(here, here, swap_send.at[a], share_recv.at[a], partner, MESH)

    def wait_all(here, sem):
        pltpu.make_async_copy(here, here, sem).wait()

    def grant(layer):
        pl.semaphore_signal(credit.at[layer], inc=1, device_id=behind[layer], device_id_type=MESH)

    def spend(layer):
        pl.semaphore_wait(credit.at[layer], 1)

    for layer in range(layers):
        prepare(0, layer).start()
    for layer in range(layers):
        first_own(0, layer).start()
    barrier = pltpu.get_barrier_semaphore()

    def greet(device):
        pl.semaphore_signal(barrier, inc=1, device_id=device, device_id_type=MESH)

    def answer(which, device):
        pl.semaphore_signal(entered.at[which], inc=1, device_id=device, device_id_type=MESH)

    def answer_chips():
        @pl.when(chip > 0)
        def _():
            answer(0, left)

        @pl.when(chip == last)
        def _():
            answer(1, right)

    greeted = jnp.where(chip > 0, 1, 0) + jnp.where(chip == last, 1, 0)
    pl.when(chip < last)(lambda: greet(right))
    pl.when(chip == 0)(lambda: greet(left))
    pl.when(core == 0)(lambda: greet(partner))
    for u in range(1, n + 1):
        for layer in range(layers):
            prepare(u, layer).start()

    @pl.when(core > 0)
    def _():
        pl.semaphore_wait(barrier, greeted + 1)
        answer(2, partner)
        answer_chips()

    @pl.when(core == 0)
    def _():
        pl.semaphore_wait(entered.at[2], 1)

    for u, (a, lo, size) in enumerate(units):
        wait_all(stage[a].at[:, pl.ds(lo, size)], stage_sem.at[u])
        for layer in range(layers):
            first_swap(u, layer).start()
        if u:
            for layer in range(layers):
                first_own(u, layer).start()
    for a, layer in pieces:
        swap(a, 1, layer, 0).start()

    @pl.when(core == 0)
    def _():
        @pl.when(chip > 0)
        def _():
            pl.semaphore_wait(barrier, greeted)

        answer_chips()

    def total(a, step, layer, i, arrived):
        t = own[a][step, layer, i].astype(jnp.float32) + pair[a][step, layer, i].astype(jnp.float32)
        if arrived is not None:
            t = t + ring[a][arrived, layer, i].astype(jnp.float32)
        return t

    def add(a, step, layer, arrived, lo, size):
        @pl.loop(lo, lo + size)
        def _(i):
            own[a][step, layer, i] = total(a, step, layer, i, arrived).astype(jnp.bfloat16)

    for u, (a, lo, size) in enumerate(units):
        wait_all(own[a].at[0, :, pl.ds(lo, size)], first_load.at[u])
        wait_all(pair[a].at[0, :, pl.ds(lo, size)], first_recv.at[u])
        for layer in range(layers):
            add(a, 0, layer, None, lo, size)

        def send(layer):
            if a < end:
                hop(a, 0, layer, lo, size).start()
                return
            hop(a, 0, layer, 0, split[layer]).start()

            @pl.when(chip != giver[layer])
            def _():
                hop(a, 0, layer, split[layer], whole - split[layer]).start()

            @pl.when(chip == giver[layer])
            def _():
                straight(layer).start()

        @pl.when(chip > 0)
        def _():
            send(1)

        if u == 0:

            @pl.when(chip < last)
            def _():
                pl.semaphore_wait(entered.at[0], 1)

        send(0)

    @pl.when(chip == 0)
    def _():
        pl.semaphore_wait(entered.at[1], 1)
        for a, lo, size in units:
            hop(a, 0, 1, lo, size).start()

    @pl.loop(1, chips)
    def _(step):
        for a, layer in pieces:
            load(a, step, layer).start()

    @pl.loop(2, chips)
    def _(step):
        for a, layer in pieces:
            swap(a, step, layer, 1).start()

    for a in range(n):
        pltpu.make_async_copy(m_in[a], new_m[a], load_sem.at[a]).start()
        pltpu.make_async_copy(v_in[a], new_v[a], load_sem.at[a]).start()
        for layer in range(layers):
            pltpu.make_async_copy(w[a].at[layer, chip, core], old_w[a].at[layer], load_sem.at[a]).start()
    for a in range(n):
        wait_all(new_w[a].at[:, pl.ds(0, (last + 1 + 4) // CORES)], load_sem.at[a])
        wait_all(pair[a].at[1], pair_recv.at[0, a])

    @pl.loop(1, last)
    def _(step):
        @pl.when(step == 2)
        def _():
            for a in range(n):
                wait_all(pair[a].at[pl.ds(2, chips - 2)], pair_recv.at[1, a])

        @pl.when(step >= SLOTS)
        def _():
            for layer in range(layers):
                spend(layer)

        for a, layer in pieces:
            if a == end:
                short = (step == 1) & (chip == 0)
                cut = split[layer]

                @pl.when(short)
                def _():
                    hop(a, 0, layer, 0, cut).wait_recv()
                    add(a, step, layer, None, cut, whole - cut)

                @pl.when(jnp.logical_not(short))
                def _():
                    hop(a, step - 1, layer).wait_recv()
                    add(a, step, layer, step - 1, cut, whole - cut)

                add(a, step, layer, step - 1, 0, cut)
            else:
                hop(a, step - 1, layer).wait_recv()
                add(a, step, layer, step - 1, 0, slabs[a])
            hop(a, step, layer).start()
            if a == end:
                grant(layer)

    def update(a, layer, lo, size, more=None):
        @pl.loop(lo, lo + size)
        def _(i):
            grad = total(a, last, layer, i, last - 1)
            if more is not None:
                grad = grad + more(i)
            grad = grad.astype(jnp.bfloat16).astype(jnp.float32)
            new = adamw(old_w[a][layer, i].astype(jnp.float32), new_m[a][layer, i], new_v[a][layer, i], grad)
            new_w[a][layer, chip, core, i], new_m[a][layer, i], new_v[a][layer, i] = new

    for layer in range(layers):
        spend(layer)
    for a, layer in pieces:
        hop(a, last - 1, layer).wait_recv()

        if a == end:
            cut = split[layer]
            update(a, layer, 0, cut)

            @pl.when(chip == taker[layer])
            def _():
                straight(layer).wait_recv()
                update(a, layer, cut, whole - cut, lambda i: extra[layer][i - cut].astype(jnp.float32))

            @pl.when(chip != taker[layer])
            def _():
                update(a, layer, cut, whole - cut)

        else:
            update(a, layer, 0, slabs[a])
        spread(a, 0, layer).start()
        share(a, 0, layer).start()
        if a == end:
            grant(layer)

            @pl.when(chip == sender[layer])
            def _():
                detour(layer).start()

    @pl.loop(1, last - 1)
    def _(step):
        for layer in range(layers):
            spend(layer)
        for a, layer in pieces:
            spread(a, step - 1, layer).wait_recv()
            spread(a, step, layer).start()
            share(a, step, layer).start()
            if a == end:

                @pl.when(step <= last - SLOTS)
                def _():
                    grant(layer)

    for layer in range(layers):
        spend(layer)
    for a, layer in pieces:
        spread(a, last - 2, layer).wait_recv()
        if a < end:
            spread(a, last - 1, layer).start()
        else:

            @pl.when(chip != keeper[layer])
            def _():
                spread_tail(last - 1, layer, 0).start()

            for k in range(1, PARTS + 1):
                spread_tail(last - 1, layer, k).start()
        share(a, last - 1, layer).start()

    for a in range(end):
        for layer in range(layers):
            spread(a, last - 1, layer).wait_recv()
            share(a, last, layer).start()
    for k in range(PARTS + 1):
        for layer in range(layers):
            spread_tail(last, layer, k).wait_recv()
            share(end, last, layer, *tail[layer][k]).start()

    for layer in range(layers):

        @pl.when(chip != keeper[layer])
        def _():
            spread_tail(last - 1, layer, 0).wait_send()

        @pl.when(chip == sender[layer])
        def _():
            detour(layer).wait_send()

        wait_all(new_w[end].at[layer, 0, 0, pl.ds(0, whole - DETOUR[layer])], tail_send.at[0, layer])
    for a in range(n):
        wait_all(new_w[a], swap_send.at[a])
        wait_all(new_w[a].at[:, pl.ds(0, last)] if a < end else ring[a], ring_send.at[a])
    wait_all(ring[end].at[pl.ds(0, last - 1)], gather_send)
    for a in range(n):
        wait_all(pair[a], share_recv.at[a])


def write(n, *refs):
    *refs, sem = refs
    sources, targets = refs[: 3 * n], refs[3 * n :]
    weights = list(zip(sources, targets, strict=True))[:n]
    for a, (source, target) in enumerate(weights):
        for layer in range(source.shape[0]):
            for chip in range(source.shape[1]):
                for core in range(source.shape[2]):
                    pltpu.make_async_copy(source.at[layer, chip, core], target.at[layer, chip, core], sem.at[a]).start()
    for source, target in zip(sources[n:], targets[n:], strict=True):
        pltpu.make_async_copy(source, target, sem.at[n]).start()
    for a, (source, target) in enumerate(weights):
        pltpu.make_async_copy(source, target, sem.at[a]).wait()
    part = sources[0].at[:, pl.ds(0, 2 * n)]
    pltpu.make_async_copy(part, part, sem.at[n]).wait()


def solution(mesh):
    chips = mesh.shape["dp"] // CORES

    def step(*arrays):
        terms, weights, m, v = (arrays[i : i + 3] for i in (0, 3, 6, 9))
        n, layers = len(terms), weights[0].shape[0]
        tiles = [(one.shape[1] // SUBLANES, SUBLANES, one.shape[2]) for one in m]
        whole = [(layers, chips, CORES, *tile) for tile in tiles]
        state = [(layers, *tile) for tile in tiles]
        operands = [one.reshape(shape) for one, shape in zip(terms, whole, strict=True)]
        operands += [one.reshape(shape) for one, shape in zip(weights, whole, strict=True)]
        operands += [one.reshape(shape) for part in (m, v) for one, shape in zip(part, state, strict=True)]
        sems = lambda *shape: pltpu.SemaphoreType.DMA(shape)
        vmem = lambda lead, dtype: [pltpu.VMEM((*lead, *tile), dtype) for tile in tiles]
        out = pl.pallas_call(
            functools.partial(kernel, n, chips, layers),
            out_shape=[pltpu.VMEM(shape, jnp.bfloat16) for shape in whole] + [pltpu.VMEM(shape, jnp.float32) for shape in state] * 2,
            in_specs=[pl.BlockSpec(memory_space=pl.ANY)] * len(operands),
            out_specs=[pl.BlockSpec(memory_space=pltpu.VMEM)] * (3 * n),
            scratch_shapes=[
                *vmem((chips, layers), jnp.bfloat16),
                *vmem((chips, layers), jnp.bfloat16),
                *vmem((chips - 1, layers), jnp.bfloat16),
                *vmem((layers,), jnp.bfloat16),
                *vmem((layers,), jnp.bfloat16),
                *[pltpu.VMEM((slabs, *tiles[-1][1:]), jnp.bfloat16) for slabs in (SEAM, LIFT)],
                sems(n + 1),
                sems(n + 1),
                sems(n),
                sems(n + 1),
                sems(2, n),
                sems(n, SLOTS, layers),
                sems(PARTS + 1, layers),
                sems(layers),
                sems(n),
                sems(n),
                sems(n),
                pltpu.SemaphoreType.DMA,
                sems(3, layers),
                pltpu.SemaphoreType.REGULAR((layers,)),
                pltpu.SemaphoreType.REGULAR((3,)),
            ],
            compiler_params=pltpu.CompilerParams(collective_id=0, has_side_effects=True, vmem_limit_bytes=40 << 20),
            name="step",
        )(*operands)
        out = pl.pallas_call(
            functools.partial(write, n),
            out_shape=[jax.ShapeDtypeStruct(one.shape, one.dtype) for one in out],
            in_specs=[pl.BlockSpec(memory_space=pltpu.VMEM)] * len(out),
            out_specs=[pl.BlockSpec(memory_space=pl.ANY)] * len(out),
            scratch_shapes=[sems(n + 1)],
            compiler_params=pltpu.CompilerParams(vmem_limit_bytes=1 << 20),
            name="write",
        )(*[pltpu.with_memory_space_constraint(one, pltpu.VMEM) for one in out])
        return tuple(one.reshape(like.shape) for one, like in zip(out, (*weights, *m, *v), strict=True))

    all_of, cut = P(None, None, None), P(None, "dp", None)
    return jax.shard_map(
        step,
        mesh=mesh,
        in_specs=(P(("rep", "dp"), None, None, None),) * 3 + (all_of,) * 3 + (cut,) * 6,
        out_specs=(P("rep", None, None),) * 3 + (P("rep", "dp", None),) * 6,
        check_vma=False,
    )
```
